32 devices in a mesh: gx: 8 (over z, y), gy: 4 (over x, core).
Axes of the slice: x: 2, y: 2, z: 4, core: 2. Of those that a mesh axis runs over, the one named last changes fastest.
Arguments:
- anomalies: float32 [80, 16, 32, 128], P(None, 'gx', 'gy'), may hold values from -6 to 6
- state_mean: float32 [16, 32, 128], P('gx', 'gy'), may hold values from -6 to 6
- obs_value: float32 [16, 256], P(None, 'gy'), may hold values from -8 to 8
- obs_cell: int32 [16, 256], replicated, may hold values from 0 to 2047
- owner: int32 [16], replicated, may hold values from 0 to 7, as said below
- order: int32 [16], replicated, may hold values from 0 to 15, each once
- root_inv: float32 [16, 256, 256], P(None, 'gy'), as said below
- gain_inv: float32 [16, 256, 256], P(None, 'gy'), as said below
Outputs:
- post_anomalies: float32 [80, 16, 32, 128], P(None, 'gx', 'gy')
- post_mean: float32 [16, 32, 128], P('gx', 'gy')
The draws below stay inside these ranges and needn't reach their ends.
Inputs may be any that keep to these rules, and one draw needn't show every extreme that they name: `owner`: some batch lies at slab 8 - 2, some at slab 1 and some at slab 8 // 2; the others favour low slabs. `order`: each batch number once. `root_inv`: symmetric. `gain_inv`: symmetric.
All inputs are finite; a program needn't handle non-finite values.
Results may differ from the reference program's by a relative error of at most 0.0001.
Values sent between devices are 32-bit elements; how exact they have to be, the bound alone decides.
A program may use at most 64 MiB of HBM per device.

```python
import math
import jax
import jax.numpy as jnp
from jax import lax

MEMBERS = 80
OBS = 256
BATCHES = 16
LON_DEV = 2
LAT_DEV = 8
LEVELS = 128
REACH = 3
NLON = 16
NLAT = 32
CELLS = 2048
N_GX = 8
N_GY = 4


def inverse_table(key, floor_value, top_value):
    key_diag, key_off = jax.random.split(key, 2)
    diagonal = jnp.exp(jax.random.uniform(key_diag, (BATCHES, OBS), jnp.float32, math.log(floor_value), math.log(top_value)))
    spread = 0.6 * math.sqrt(floor_value * top_value) / math.sqrt(OBS)
    offdiag_noise = jax.random.normal(key_off, (BATCHES, OBS, OBS), jnp.float32) * spread
    inverse = 0.5 * (offdiag_noise + jnp.swapaxes(offdiag_noise, 1, 2)) + diagonal[:, :, None] * jnp.eye(OBS, dtype=jnp.float32)
    return inverse


def draw_root_inv(key, part):
    return inverse_table(jax.random.fold_in(key, 11), 0.15, 0.5)


def draw_gain_inv(key, part):
    return inverse_table(jax.random.fold_in(key, 23), 0.3, 0.9)


def draw_owner(key, part):
    key_first, key_second, key_perm = jax.random.split(jax.random.fold_in(key, 37), 3)
    first_draw = jax.random.randint(key_first, (BATCHES,), 0, N_GX, dtype=jnp.int32)
    second_draw = jax.random.randint(key_second, (BATCHES,), 0, N_GX, dtype=jnp.int32)
    slabs = jnp.minimum(first_draw, second_draw)
    anchors = jnp.array([N_GX - 2, 1, N_GX // 2], dtype=jnp.int32)
    slabs = slabs.at[:3].set(anchors)
    shuffle = jax.random.permutation(key_perm, BATCHES)
    return slabs[shuffle].astype(jnp.int32)


def place_ends(drawn, own_key, least, high):
    index_at = [jax.random.randint(jax.random.fold_in(own_key, axis), (), 0, length) for axis, length in enumerate(drawn.shape)]
    longest = drawn.shape.index(max(drawn.shape))
    neighbour = index_at[:longest] + [(index_at[longest] + 1) % drawn.shape[longest]] + index_at[longest + 1:]
    return drawn.at[tuple(index_at)].set(least).at[tuple(neighbour)].set(high)


def block_levels(own_key, shape, cuts, low, largest):
    loudness = 1.0
    for dim, parts in cuts:
        draws = jax.random.uniform(jax.random.fold_in(jax.random.fold_in(own_key, 6), dim), (parts,), jnp.float32, low / len(cuts), largest / len(cuts))
        loudness = loudness * jnp.repeat(jnp.exp(draws), shape[dim] // parts).reshape((-1,) + (1,) * (len(shape) - 1 - dim))
    return loudness


def noise(key, dims, deviation, most, shards=(), kind=jnp.bfloat16):
    level = block_levels(key, dims, shards, -0.22, 0.18) if shards else 1.0
    drawn = jax.random.normal(key, dims, jnp.float32) * deviation * level
    return jnp.minimum(jnp.maximum(drawn, -most), most).astype(kind)


def setup_inputs(seed: int = 0) -> dict:
    arg_keys = jax.random.split(jax.random.key(seed), 9)
    anomalies = noise(arg_keys[0], (MEMBERS, NLON, NLAT, LEVELS), 1.0, 6.0, ((1, 8), (2, 4)), jnp.float32)
    state_mean = noise(arg_keys[1], (NLON, NLAT, LEVELS), 1.0, 6.0, ((0, 8), (1, 4)), jnp.float32)
    obs_value = noise(arg_keys[2], (BATCHES, OBS), 1.5, 8.0, ((1, 4),), jnp.float32)
    obs_cell = place_ends(jax.random.randint(arg_keys[3], (BATCHES, OBS), 0, CELLS), jax.random.fold_in(arg_keys[3], 1), 0, CELLS - 1).astype(jnp.int32)
    owner = draw_owner(jax.random.fold_in(arg_keys[8], 71), 0)
    order = jax.random.permutation(arg_keys[5], BATCHES).astype(jnp.int32)
    root_inv = draw_root_inv(jax.random.fold_in(arg_keys[8], 71), 0)
    gain_inv = draw_gain_inv(jax.random.fold_in(arg_keys[8], 71), 0)
    return {"anomalies": anomalies, "state_mean": state_mean, "obs_value": obs_value, "obs_cell": obs_cell, "owner": owner, "order": order, "root_inv": root_inv, "gain_inv": gain_inv}


def product(left_side, right_side):
    return jnp.dot(left_side, right_side, precision=lax.Precision.HIGHEST, preferred_element_type=jnp.float32)


def reference(anomalies, state_mean, obs_value, obs_cell, owner, order, root_inv, gain_inv):
    lon_total = LON_DEV * N_GX
    lat_total = LAT_DEV * N_GY
    quarter = OBS // N_GY
    window_width = (2 * REACH + 1) * LON_DEV
    reach_cells = REACH * LON_DEV
    taper_span = REACH * LON_DEV + 1.0
    obs_band = jnp.arange(OBS, dtype=jnp.int32) // quarter
    lat_index = jnp.arange(lat_total, dtype=jnp.int32)
    offsets = jnp.arange(window_width, dtype=jnp.int32)

    def assimilate(batch_turn, carried):
        state_field, mean_field = carried
        batch_id = order[batch_turn]
        root_slab = owner[batch_id]
        cells_of = obs_cell[batch_id]
        obs_lon = root_slab * LON_DEV + cells_of // (LAT_DEV * LEVELS)
        obs_lat = obs_band * LAT_DEV + (cells_of // LEVELS) % LAT_DEV
        obs_lev = cells_of % LEVELS
        prior_all = state_field[:, obs_lon, obs_lat, obs_lev]
        innovation = obs_value[batch_id] - mean_field[obs_lon, obs_lat, obs_lev]
        weighted = product(prior_all, root_inv[batch_id].T)
        gain_vec = product(gain_inv[batch_id], innovation)
        window_lon = (root_slab * LON_DEV - reach_cells + offsets) % lon_total
        window = state_field[:, window_lon].reshape(MEMBERS, -1)
        mean_window = mean_field[window_lon].reshape(-1)
        cell_lon = jnp.broadcast_to(window_lon[:, None, None], (window_width, lat_total, LEVELS)).reshape(-1)
        cell_lat = jnp.broadcast_to(lat_index[None, :, None], (window_width, lat_total, LEVELS)).reshape(-1)
        lon_gap = jnp.abs(obs_lon[:, None] - cell_lon[None, :])
        cycle_gap = jnp.minimum(lon_gap, lon_total - lon_gap)
        lat_gap = jnp.abs(obs_lat[:, None] - cell_lat[None, :])
        taper_rows = jnp.maximum(0.0, 1.0 - cycle_gap.astype(jnp.float32) / taper_span) * (1.0 - lat_gap.astype(jnp.float32) / lat_total)
        covariance = product(prior_all.T, window) / (MEMBERS - 1.0)
        gained = taper_rows * covariance
        stacked = jnp.concatenate([weighted, gain_vec[None, :]], axis=0)
        increment = product(stacked, gained)
        new_window = (window - increment[:MEMBERS]).reshape(MEMBERS, window_width, lat_total, LEVELS)
        new_mean = (mean_window + increment[MEMBERS]).reshape(window_width, lat_total, LEVELS)
        state_field = state_field.at[:, window_lon].set(new_window)
        mean_field = mean_field.at[window_lon].set(new_mean)
        return state_field, mean_field

    post_anomalies, post_mean = lax.fori_loop(0, BATCHES, assimilate, (anomalies, state_mean))
    return post_anomalies, post_mean
```

```python
import functools

import jax
import jax.numpy as jnp
from jax import lax
from jax.experimental import pallas as pl
from jax.experimental.pallas import tpu as pltpu
from jax.sharding import PartitionSpec as P

REACH = 3
EARLY = 5
LANES = 128
MESH = pl.DeviceIdType.MESH
VMEM = pl.BlockSpec(memory_space=pltpu.VMEM)
SMEM = pl.BlockSpec(memory_space=pltpu.SMEM)
F32 = jnp.float32
BF16 = jnp.bfloat16


def split(value):
    high = value.astype(BF16)
    return high, (value - high.astype(F32)).astype(BF16)


def nn(left, right):
    return lax.dot_general(left, right, (((1,), (0,)), ((), ())), preferred_element_type=F32)


def nt(left, right):
    return lax.dot_general(left, right, (((1,), (1,)), ((), ())), preferred_element_type=F32)


def lane_ids(shape):
    return lax.broadcasted_iota(jnp.int32, shape, len(shape) - 1)


def pick_kernel(lon_dev, lat_dev, cells_ref, value_ref, owner_ref, order_ref, anom_ref, mean_ref, state_ref, packed_ref, rows_ref):
    column, band = lax.axis_index("gx"), lax.axis_index("gy")
    members, classes, levels = anom_ref.shape
    batches, quarter = value_ref.shape

    for c in range(classes):
        lat = (band * lat_dev + c % lat_dev).astype(F32)
        lon = (column * lon_dev + c // lat_dev).astype(F32)
        tall = jnp.concatenate(
            [
                anom_ref[:, c, :],
                mean_ref[pl.ds(c, 1), :],
                jnp.full((1, levels), lat, F32),
                jnp.full((1, levels), lon, F32),
                jnp.zeros((LANES - members - 3, levels), F32),
            ],
            axis=0,
        )
        state_ref[pl.ds(c * levels, levels), :] = tall.T

    lane = lane_ids((1, LANES))

    def batch(t, _):
        b = order_ref[t]
        mine = owner_ref[b] == column

        @pl.when(mine)
        def _():
            def group(i, _):
                for k in range(8):
                    j = i * 8 + k
                    row = state_ref[pl.ds(cells_ref[b, band * quarter + j], 1), :]
                    rows_ref[pl.ds(t * quarter + j, 1), :] = jnp.where(lane == members + 3, value_ref[b, j], row)
                return 0

            lax.fori_loop(0, quarter // 8, group, 0)

        @pl.when(jnp.logical_not(mine))
        def _():
            rows_ref[pl.ds(pl.multiple_of(t * quarter, quarter), quarter), :] = jnp.zeros((quarter, LANES), F32)

        return 0

    lax.fori_loop(0, batches, batch, 0)
    slabs, height, chunk = packed_ref.shape
    for q in range(slabs):
        packed_ref[q] = rows_ref[pl.ds(q * chunk, chunk), :].T[:height]


def spread_kernel(bands, slabs, rows_ref, out_ref, land, send1, recv1, send2, recv2, send3, recv3, send4, recv4, send5, recv5):
    x, b = lax.axis_index("gx"), lax.axis_index("gy")
    partner = b + 1 - 2 * lax.rem(b, 2)
    across = lax.rem(b + 2, bands)

    def slab(k):
        return lax.rem(x + k, slabs)

    def source(k):
        return lax.rem(x + slabs - k, slabs)

    def first(k):
        return pltpu.make_async_remote_copy(
            src_ref=rows_ref.at[slab(k)], dst_ref=land.at[k], send_sem=send1.at[k], recv_sem=recv1.at[k],
            device_id={"gx": slab(k)}, device_id_type=MESH,
        )

    def second(k):
        return pltpu.make_async_remote_copy(
            src_ref=out_ref.at[b, x], dst_ref=out_ref.at[b, x], send_sem=send2.at[k],
            recv_sem=recv2.at[k], device_id={"gx": slab(k)}, device_id_type=MESH,
        )

    def hand(k, of_band, send_sem, recv_sem, target):
        place = out_ref.at[of_band, source(k)]
        return pltpu.make_async_remote_copy(
            src_ref=place, dst_ref=place, send_sem=send_sem.at[k], recv_sem=recv_sem.at[k],
            device_id={"gy": target}, device_id_type=MESH,
        )

    def third(k):
        return hand(k, b, send3, recv3, partner)

    def fourth(k):
        return hand(k, b, send4, recv4, across)

    def fifth(k):
        return hand(k, across, send5, recv5, partner)

    def each(low, high, body):
        def step(k, _):
            body(k)
            return 0

        lax.fori_loop(low, high, step, 0)

    barrier = pltpu.get_barrier_semaphore()
    each(1, slabs, lambda k: pl.semaphore_signal(barrier, inc=1, device_id={"gx": slab(k)}, device_id_type=MESH))
    for target in (partner, across):
        pl.semaphore_signal(barrier, inc=1, device_id={"gy": target}, device_id_type=MESH)
    pl.semaphore_wait(barrier, slabs + 1)

    each(1, slabs, lambda k: first(k).start())
    out_ref[b, x] = rows_ref[x]

    def add(k):
        first(k).wait_recv()
        out_ref[b, x] += land[k]

    each(1, slabs, add)
    fourth(0).start()
    each(1, slabs, lambda k: second(k).start())
    third(0).start()

    def relay(k):
        second(k).wait_recv()
        fourth(k).start()
        third(k).start()
        fourth(k - 1).wait_recv()
        fifth(k - 1).start()

    each(1, slabs, relay)
    fourth(slabs - 1).wait_recv()
    fifth(slabs - 1).start()

    def finish(k):
        third(k).wait()
        fifth(k).wait()
        fourth(k).wait_send()

    each(0, slabs, finish)

    def sent(k):
        first(k).wait_send()
        second(k).wait_send()

    each(1, slabs, sent)


def main_kernel(
    sizes, order_ref, owner_ref, state_ref, obs_ref, cell_ref, root_ref, gain_ref,
    anom_out, mean_out,
    lat_ref, lon_ref, cells_s, obs_s, v_s, vw_s, z3_s, gh_s, gl_s, send_sem, recv_sem,
):
    members, lon_dev, lat_dev, levels, lon_total, lat_total, span, bands = sizes
    batches, obs = cell_ref.shape
    quarter = obs // bands
    column, band = lax.axis_index("gx"), lax.axis_index("gy")
    classes = lon_dev * lat_dev
    chunk = 4

    barrier = pltpu.get_barrier_semaphore()
    for k in range(1, bands):
        pl.semaphore_signal(barrier, inc=1, device_id={"gy": lax.rem(band + k, bands)}, device_id_type=MESH)
    pl.semaphore_wait(barrier, bands - 1)

    def widen(value, with_low_in_middle):
        high, low = split(value)
        high, low = high.astype(F32), low.astype(F32)
        second, third = (low, high) if with_low_in_middle else (high, low)
        lane = lane_ids(value.shape)
        room = LANES - members
        moved = pltpu.roll(second, members, 1)
        first = jnp.where(lane < members, high, moved)
        last = jnp.where(lane < members - room, moved, pltpu.roll(third, members - room, 1))
        return jnp.concatenate([first, last], axis=1), lane, room

    def state_wide(value):
        return widen(value, True)[0].astype(BF16)

    def prior_wide(value):
        wide, lane, room = widen(jnp.where(lane_ids(value.shape) < members, value, 0.0), False)
        wide_lane = lane_ids(wide.shape)
        return jnp.where(wide_lane < 3 * members, wide, 0.0).astype(BF16)

    def lon_weight(gap):
        gap = jnp.abs(gap)
        gap = jnp.minimum(gap, lon_total - gap)
        return jnp.maximum(0.0, 1.0 - gap * (1.0 / span))

    def lat_weight(gap):
        return 1.0 - jnp.abs(gap) * (1.0 / lat_total)

    def obs_taper(rows, s):
        lat, lon = rows[:, members + 1:members + 2], rows[:, members + 2:members + 3]
        return lat_weight(lat - lat_ref[s]) * lon_weight(lon - lon_ref[s])

    def apply(rows, high, low):
        both = nn(high, vw_s[...])
        return rows - (both[:, :LANES] + both[:, LANES:] + nn(low, vw_s[:, :LANES]))

    def update(rows, taper, s, slot):
        gained = nt(state_wide(rows), z3_s[slot]) * taper
        return apply(rows, *split(gained))

    def update_cells(s, slot):
        for i in range(classes // chunk):
            tapers = []
            for k in range(chunk):
                c = i * chunk + k
                lat = (band * lat_dev + c % lat_dev).astype(F32)
                lon = (column * lon_dev + c // lat_dev).astype(F32)
                weight = lat_weight(lat - lat_ref[s]) * lon_weight(lon - lon_ref[s])
                tapers.append(jnp.broadcast_to(weight, (levels, obs)))
            here = pl.ds(i * chunk * levels, chunk * levels)
            cells_s[here, :] = update(cells_s[here, :], jnp.concatenate(tapers, axis=0), s, slot)

    def at(t):
        return pl.ds(pl.multiple_of(t * obs, obs), obs)

    cells_s[...] = state_ref[...]
    _, slabs, height, width = obs_ref.shape
    part = min(width, quarter)
    for q in range(bands):
        for p in range(slabs):
            rest = jnp.zeros((LANES - height, width), F32)
            block = jnp.concatenate([obs_ref[q, p], rest], axis=0).T
            for i in range(0, width, part):
                t, j = divmod(p * width + i, quarter)
                obs_s[pl.ds(t * obs + q * quarter + j, part), :] = block[i:i + part]
    obs_s[pl.ds(batches * obs, 2 * obs), :] = jnp.zeros((2 * obs, LANES), F32)
    vw_s[...] = jnp.zeros_like(vw_s)
    z3_s[...] = jnp.zeros_like(z3_s)
    first_lat = lax.broadcasted_iota(jnp.int32, (1, obs), 1).astype(F32)
    first_lat = jnp.floor((first_lat + 0.5) * (1.0 / quarter)) * lat_dev
    for t in range(batches):
        batch_id = order_ref[t]
        level_row = jnp.floor((cell_ref[pl.ds(batch_id, 1), :].astype(F32) + 0.5) * (1.0 / levels))
        lon_row = jnp.floor((level_row + 0.5) * (1.0 / lat_dev))
        lat_ref[t] = level_row - lon_row * lat_dev + first_lat
        lon_ref[t] = lon_row + (owner_ref[batch_id] * lon_dev).astype(F32)

    def turn(t, _):
        prior = obs_s[at(t), :]
        lane = lane_ids(prior.shape)
        innovation = pltpu.roll(prior, LANES - 3, 1) - prior
        joined = jnp.where(lane < members, prior, jnp.where(lane == members, innovation, 0.0))
        high, low = split(joined)
        batch_id = order_ref[t]
        table_high, table_low = split(jnp.concatenate([root_ref[batch_id], gain_ref[batch_id]], axis=0))
        both = nn(table_high, jnp.concatenate([high, low], axis=1))
        part = both[:, :LANES] + both[:, LANES:] + nn(table_low, high)
        lane = lane_ids((quarter, LANES))
        weighted = jnp.where(lane < members, part[:quarter], jnp.where(lane == members, -part[quarter:], 0.0))
        mine = pl.ds(pl.multiple_of(band * quarter, quarter), quarter)
        v_s[t, mine, :] = weighted * (1.0 / (members - 1.0))

        def copy(k):
            return pltpu.make_async_remote_copy(
                src_ref=v_s.at[t, mine, :],
                dst_ref=v_s.at[t, mine, :],
                send_sem=send_sem.at[t, k - 1],
                recv_sem=recv_sem.at[t, k - 1],
                device_id={"gy": lax.rem(band + k, bands)},
                device_id_type=MESH,
            )

        for k in range(1, bands):
            copy(k).start()

        z3_s[lax.rem(t, 2)] = prior_wide(prior)

        before = jnp.maximum(t - 1, 0)
        past = lax.rem(t + 1, 2)
        rows = obs_s[at(t + 1), :]
        rows = update(rows, obs_taper(rows, before), before, past)
        obs_s[at(t + 1), :] = rows
        gained = nt(state_wide(rows), z3_s[lax.rem(t, 2)]) * obs_taper(rows, t)
        gh_s[...], gl_s[...] = split(gained)
        update_cells(before, past)

        def later(i, _):
            here = pl.ds(pl.multiple_of((t + 2 + 2 * i) * obs, obs), 2 * obs)
            rows = obs_s[here, :]
            obs_s[here, :] = update(rows, obs_taper(rows, before), before, past)
            return 0

        lax.fori_loop(0, (batches - 1 - t) // 2 * jnp.minimum(t, 1), later, 0)

        for k in range(1, bands):
            copy(k).wait()

        vw_s[...] = jnp.concatenate(split(v_s[t]), axis=1)

        obs_s[at(t + 1), :] = apply(obs_s[at(t + 1), :], gh_s[...], gl_s[...])
        return 0

    lax.fori_loop(0, batches, turn, 0)
    update_cells(batches - 1, (batches - 1) % 2)
    for c in range(classes):
        tall = cells_s[pl.ds(c * levels, levels), :].T
        anom_out[:, c, :] = tall[:members]
        mean_out[pl.ds(c, 1), :] = tall[members:members + 1]


def wide_local(anomalies, state_mean, obs_value, obs_cell, owner, order, root_inv, gain_inv):
    members, lon_dev, lat_dev, levels = anomalies.shape
    classes = lon_dev * lat_dev
    cells = classes * levels
    batches, quarter = obs_value.shape
    obs = obs_cell.shape[1]
    slabs, bands = lax.axis_size("gx"), lax.axis_size("gy")
    chunk = batches * quarter // slabs
    height = (members + 4 + 7) // 8 * 8
    state, rows = pl.pallas_call(
        functools.partial(pick_kernel, lon_dev, lat_dev),
        out_shape=(
            jax.ShapeDtypeStruct((cells, LANES), F32),
            jax.ShapeDtypeStruct((slabs, height, chunk), F32),
        ),
        in_specs=[SMEM] * 4 + [VMEM] * 2,
        out_specs=(VMEM, VMEM),
        scratch_shapes=[pltpu.VMEM((batches * quarter, LANES), F32)],
        name="pick",
    )(
        obs_cell, obs_value, owner, order,
        anomalies.reshape(members, classes, levels), state_mean.reshape(classes, levels),
    )

    rows = pl.pallas_call(
        functools.partial(spread_kernel, bands, slabs),
        out_shape=jax.ShapeDtypeStruct((bands, slabs, height, chunk), F32),
        in_specs=[VMEM],
        out_specs=VMEM,
        scratch_shapes=[pltpu.VMEM((slabs, height, chunk), F32)] + [pltpu.SemaphoreType.DMA((slabs,))] * 10,
        compiler_params=pltpu.CompilerParams(collective_id=1, has_side_effects=True),
        name="spread",
    )(rows)

    sizes = (
        members, lon_dev, lat_dev, levels, float(slabs * lon_dev), float(bands * lat_dev), REACH * lon_dev + 1.0, bands
    )
    post, mean = pl.pallas_call(
        functools.partial(main_kernel, sizes),
        out_shape=(
            jax.ShapeDtypeStruct((members, classes, levels), F32),
            jax.ShapeDtypeStruct((classes, levels), F32),
        ),
        in_specs=[SMEM] * 2 + [VMEM] * 5,
        out_specs=(VMEM, VMEM),
        scratch_shapes=[
            pltpu.VMEM((batches, 1, obs), F32),
            pltpu.VMEM((batches, 1, obs), F32),
            pltpu.VMEM((cells, LANES), F32),
            pltpu.VMEM(((batches + 2) * obs, LANES), F32),
            pltpu.VMEM((batches, obs, LANES), F32),
            pltpu.VMEM((obs, 2 * LANES), BF16),
            pltpu.VMEM((2, obs, 2 * LANES), BF16),
            pltpu.VMEM((obs, obs), BF16),
            pltpu.VMEM((obs, obs), BF16),
            pltpu.SemaphoreType.DMA((batches, bands - 1)),
            pltpu.SemaphoreType.DMA((batches, bands - 1)),
        ],
        compiler_params=pltpu.CompilerParams(collective_id=0, has_side_effects=True),
        name="analysis",
    )(
        order, owner, state, rows, obs_cell, root_inv, gain_inv,
    )
    return post.reshape(members, lon_dev, lat_dev, levels), mean.reshape(lon_dev, lat_dev, levels)


def arrange_kernel(
    lon_dev, lat_dev, lat_total, cells_ref, value_ref, owner_ref, order_ref, anom_ref, mean_ref, root_ref, gain_ref,
    state_ref, packed_ref, table_ref,
):
    column, band = lax.axis_index("gx"), lax.axis_index("gy")
    members, classes, levels = anom_ref.shape
    batches, quarter = value_ref.shape
    slabs, height, _ = packed_ref.shape
    piece = height // batches
    half = table_ref.shape[-1]

    for c in range(classes):
        lat = (band * lat_dev + c % lat_dev).astype(F32) * (1.0 / lat_total)
        lon = (column * lon_dev + c // lat_dev).astype(F32)
        tall = jnp.concatenate(
            [
                anom_ref[:, c, :],
                mean_ref[pl.ds(c, 1), :],
                jnp.full((1, levels), lat, F32),
                jnp.full((1, levels), lon, F32),
                jnp.zeros((1, levels), F32),
                jnp.full((1, levels), float(c // lat_dev), F32),
                jnp.zeros((LANES - members - 5, levels), F32),
            ],
            axis=0,
        )
        state_ref[pl.ds(c * levels, levels), :] = tall.T

    lane = lane_ids((1, LANES))

    def batch(t, _):
        b = order_ref[t]
        mine = owner_ref[b] == column
        for h in range(2):
            table_ref[t, 0, h] = root_ref[b, :, h * half:(h + 1) * half]
            table_ref[t, 1, h] = gain_ref[b, :, h * half:(h + 1) * half]

        @pl.when(mine)
        def _():
            def group(p, _):
                for k in range(piece):
                    j = p * piece + k
                    row = state_ref[pl.ds(cells_ref[b, band * quarter + j], 1), :]
                    packed_ref[p, pl.ds(t * piece + k, 1), :] = jnp.where(lane == members + 3, value_ref[b, j], row)
                return 0

            lax.fori_loop(0, slabs, group, 0)

        @pl.when(jnp.logical_not(mine))
        def _():
            here = pl.ds(pl.multiple_of(t * piece, piece), piece)
            packed_ref[:, here, :] = jnp.zeros((slabs, piece, LANES), F32)

        return 0

    lax.fori_loop(0, batches, batch, 0)


def analysis_kernel(
    sizes, order_ref, owner_ref, state_ref, packed_ref, table_ref, cell_ref,
    cells_s,
    lat_ref, lon_ref, land, mine_s, share_s, obs_s, full_s, th_s, tl_s, z3_s, vw_s,
    rs_send, rs_recv, send1, recv1, send2, recv2, near_send, near_recv, far_send, far_recv, hand_send, hand_recv, own_sem,
):
    members, lon_dev, lat_dev, levels, lon_total, lat_total, span, bands, slabs, early = sizes
    batches, obs = cell_ref.shape
    quarter, half = obs // bands, obs // 2
    piece = quarter // slabs
    ahead, first_tables = min(5, batches), min(3, batches)
    column, band = lax.axis_index("gx"), lax.axis_index("gy")
    partner = band + 1 - 2 * lax.rem(band, 2)
    across = lax.rem(band + bands // 2, bands)
    near = lax.div(band, bands // 2)
    far = 1 - near
    classes = lon_dev * lat_dev
    chunk = 4

    def slab(k):
        return lax.rem(column + k, slabs)

    def band_rows(b):
        return pl.ds(pl.multiple_of(b * quarter, quarter), quarter)

    def half_rows(h):
        return pl.ds(pl.multiple_of(h * half, half), half)

    def remote(src, dst, send, recv, device):
        return pltpu.make_async_remote_copy(
            src_ref=src, dst_ref=dst, send_sem=send, recv_sem=recv, device_id=device, device_id_type=MESH
        )

    parts = ((0, early * piece), (early * piece, (batches - early) * piece))

    def reduce_copy(k, p):
        here = pl.ds(*parts[p])
        return remote(
            packed_ref.at[slab(k), here], land.at[k, here], rs_send.at[p, k], rs_recv.at[p, k], {"gx": slab(k)}
        )

    def my_piece(s):
        return pl.ds(pl.multiple_of(s * piece, piece), piece)

    def my_place():
        return pl.ds(pl.multiple_of(band * quarter + column * piece, piece), piece)

    def share(s):
        rows = mine_s[my_piece(s), :]
        share_s[s] = rows
        obs_s[s, my_place(), :] = rows

        def start(device):
            remote(share_s.at[s], obs_s.at[s, my_place()], send1.at[s], recv1.at[s], device).start()

        for k in range(1, slabs):
            start({"gx": slab(k)})
        for k in range(slabs):
            start({"gx": slab(k), "gy": across})

    def shared(s, sem):
        window = obs_s.at[s, pl.ds(0, (2 * slabs - 1) * piece)]
        pltpu.make_async_copy(window, window, sem.at[s]).wait()

    def pass_on(s, i):
        place = obs_s.at[s, band_rows((band, across)[i])]
        return remote(place, place, send2.at[s, i], recv2.at[s, i], {"gy": partner})

    def near_copy(t):
        return remote(
            table_ref.at[t], full_s.at[t, :, :, band_rows(band)], near_send.at[t], near_recv.at[t], {"gy": partner}
        )

    def far_copy(t):
        return remote(
            table_ref.at[t, :, near], full_s.at[t, :, near, band_rows(band)], far_send.at[t], far_recv.at[t],
            {"gy": across},
        )

    def hand_copy(t):
        place = full_s.at[t, :, far, band_rows(across)]
        return remote(place, place, hand_send.at[t], hand_recv.at[t], {"gy": partner})

    def send_table(t):
        far_copy(t).start()
        near_copy(t).start()

    def hand_table(t):
        far_copy(t).wait_recv()
        hand_copy(t).start()

    def own_tables():
        return pltpu.make_async_copy(table_ref, full_s.at[:, :, :, band_rows(band)], own_sem)

    def prepare(t, slot):
        for k in range(2):
            aside = full_s[t, k, far, half_rows(near), :]
            blocks = (
                (near, near, full_s[t, k, near, half_rows(near), :]),
                (far, near, aside),
                (near, far, aside.T),
                (far, far, full_s[t, k, far, half_rows(far), :]),
            )
            for columns, rows, block in blocks:
                here = pl.ds(pl.multiple_of(k * obs + rows * half, half), half)
                high, low = split(block)
                th_s[slot, columns, here, :] = high
                tl_s[slot, columns, here, :] = low

    barrier = pltpu.get_barrier_semaphore()
    for k in range(1, slabs):
        pl.semaphore_signal(barrier, inc=1, device_id={"gx": slab(k)}, device_id_type=MESH)
    for k in range(slabs):
        pl.semaphore_signal(barrier, inc=1, device_id={"gx": slab(k), "gy": across}, device_id_type=MESH)
    pl.semaphore_signal(barrier, inc=1, device_id={"gy": partner}, device_id_type=MESH)
    pl.semaphore_wait(barrier, 2 * slabs)

    for p in range(2):
        for k in range(1, slabs):
            reduce_copy(k, p).start()
        if p == 0:
            own_tables().start()
            for t in range(first_tables):
                send_table(t)

    first_lat = lax.broadcasted_iota(jnp.int32, (1, obs), 1).astype(F32)
    first_lat = jnp.floor((first_lat + 0.5) * (1.0 / quarter)) * lat_dev
    for t in range(batches):
        batch_id = order_ref[t]
        level_row = jnp.floor((cell_ref[pl.ds(batch_id, 1), :].astype(F32) + 0.5) * (1.0 / levels))
        lon_row = jnp.floor((level_row + 0.5) * (1.0 / lat_dev))
        lat_ref[t + early] = (level_row - lon_row * lat_dev + first_lat) * (1.0 / lat_total)
        lon_ref[t + early] = lon_row + (owner_ref[batch_id] * lon_dev).astype(F32)
    for t in range(early):
        lat_ref[t] = jnp.zeros((1, obs), F32)
        lon_ref[t] = jnp.zeros((1, obs), F32)
        vw_s[t] = jnp.zeros(vw_s.shape[1:], BF16)
        z3_s[t] = jnp.zeros(z3_s.shape[1:], BF16)
    for s in range(batches, obs_s.shape[0]):
        obs_s[s] = jnp.zeros(obs_s.shape[1:], F32)
    cells_s[...] = state_ref[...]

    def collect(p):
        here = pl.ds(*parts[p])
        total = packed_ref[column, here, :]
        for k in range(1, slabs):
            reduce_copy(k, p).wait_recv()
            total = total + land[k, here, :]
        mine_s[here, :] = total

    collect(0)
    for s in range(early):
        share(s)
    for t in range(first_tables, ahead):
        send_table(t)
    for t in range(min(3, batches)):
        hand_table(t)
    collect(1)
    for s in range(early):
        shared(s, recv1)
        for i in range(2):
            pass_on(s, i).start()
    own_tables().wait()
    near_copy(0).wait_recv()
    hand_copy(0).wait_recv()
    prepare(0, 0)
    for s in range(early):
        for i in range(2):
            pass_on(s, i).wait()

    def state_wide(value):
        high, low = split(value)
        high, low = high.astype(F32), low.astype(F32)
        lane = lane_ids(value.shape)
        room = LANES - members
        moved = pltpu.roll(low, members, 1)
        first = jnp.where(lane < members, high, moved)
        last = jnp.where(lane < members - room, moved, pltpu.roll(high, members - room, 1))
        return jnp.concatenate([first, last], axis=1).astype(BF16)

    def prior_tall(prior):
        high, low = split(prior.T[:members])
        return jnp.concatenate([high, high, low, jnp.zeros((2 * LANES - 3 * members, obs), BF16)], axis=0)

    def lon_weight(gap):
        gap = jnp.abs(gap)
        gap = jnp.minimum(gap, lon_total - gap)
        return jnp.maximum(0.0, 1.0 - gap * (1.0 / span))

    def lat_weight(gap):
        return 1.0 - jnp.abs(gap)

    def apply(rows, high, low, e):
        both = nn(high, vw_s[e])
        return rows - (both[:, :LANES] + both[:, LANES:] + nn(low, vw_s[e, :, :LANES]))

    def gain_of(rows, taper, e):
        return split(nn(state_wide(rows), z3_s[e]) * taper)

    def update(rows, taper, e):
        high, low = gain_of(rows, taper, e)
        return apply(rows, high, low, e)

    def obs_taper(lat, bit, s, e):
        lon = (owner_ref[order_ref[jnp.minimum(s, batches - 1)]] * lon_dev).astype(F32)
        west = lon_weight(lon - lon_ref[e])
        east = lon_weight(lon + 1.0 - lon_ref[e])
        return lat_weight(lat - lat_ref[e]) * (west + bit * (east - west))

    def update_mine(e):
        rows = mine_s[...]
        lat, lon = rows[:, members + 1:members + 2], rows[:, members + 2:members + 3]
        taper = lat_weight(lat - lat_ref[e]) * lon_weight(lon - lon_ref[e])
        mine_s[...] = update(rows, taper, e)

    def update_cells(e):
        for i in range(classes // chunk):
            tapers = []
            for k in range(chunk):
                c = i * chunk + k
                lat = (band * lat_dev + c % lat_dev).astype(F32) * (1.0 / lat_total)
                lon = (column * lon_dev + c // lat_dev).astype(F32)
                weight = lat_weight(lat - lat_ref[e]) * lon_weight(lon - lon_ref[e])
                tapers.append(jnp.broadcast_to(weight, (levels, obs)))
            here = pl.ds(i * chunk * levels, chunk * levels)
            cells_s[here, :] = update(cells_s[here, :], jnp.concatenate(tapers, axis=0), e)

    def columns_of(rows):
        return rows[:, members + 1:members + 2], rows[:, members + 4:members + 5]

    def turn(t, _):
        slot = lax.rem(t, 2)
        e = t + early

        @pl.when(e < batches)
        def _():
            share(e)

        passing = e - 2

        @pl.when(jnp.logical_and(passing >= early, passing < batches))
        def _():
            shared(passing, recv1)
            for i in range(2):
                pass_on(passing, i).start()

        @pl.when(t + ahead < batches)
        def _():
            send_table(t + ahead)

        @pl.when(t + 3 < batches)
        def _():
            hand_table(t + 3)

        @pl.when(t + 1 < batches)
        def _():
            near_copy(t + 1).wait_recv()
            hand_copy(t + 1).wait_recv()

        coming = t + 2

        @pl.when(jnp.logical_and(coming >= early, coming < batches))
        def _():
            for i in range(2):
                pass_on(coming, i).wait()

        prior = obs_s[t]
        z3_s[e] = prior_tall(prior)
        lane = lane_ids(prior.shape)
        innovation = pltpu.roll(prior, LANES - 3, 1) - prior
        joined = jnp.where(lane < members, prior, jnp.where(lane == members, innovation, 0.0))
        high, low = split(joined)
        table_high = jnp.concatenate([th_s[slot, 0], th_s[slot, 1]], axis=1)
        table_low = jnp.concatenate([tl_s[slot, 0], tl_s[slot, 1]], axis=1)
        both = nn(table_high, jnp.concatenate([high, low], axis=1))
        part = both[:, :LANES] + both[:, LANES:] + nn(table_low, high)
        lane = lane_ids((obs, LANES))
        weighted = jnp.where(lane < members, part[:obs], jnp.where(lane == members, -part[obs:], 0.0))
        vw_s[e] = jnp.concatenate(split(weighted * (1.0 / (members - 1.0))), axis=1)

        rows = obs_s[t + 1]
        lat, bit = columns_of(rows)
        gained = gain_of(rows, obs_taper(lat, bit, t + 1, e), e)

        update_cells(e - 1)

        obs_s[t + 1] = apply(rows, *gained, e)
        update_mine(e)

        rows = obs_s[t + 2]
        lat, bit = columns_of(rows)
        for k in range(early - 2, -1, -1):
            rows = update(rows, obs_taper(lat, bit, t + 2, e - k), e - k)
        obs_s[t + 2] = rows

        prepare(jnp.minimum(t + 1, batches - 1), 1 - slot)
        return 0

    lax.fori_loop(0, batches, turn, 0)
    update_cells(batches - 1 + early)

    for p in range(2):
        for k in range(1, slabs):
            reduce_copy(k, p).wait_send()

    def sent(t, _):
        shared(t, send1)
        near_copy(t).wait_send()
        far_copy(t).wait_send()
        hand_copy(t).wait_send()
        return 0

    lax.fori_loop(0, batches, sent, 0)


def finish_kernel(cells_ref, anom_out, mean_out):
    members, classes, levels = anom_out.shape
    for c in range(classes):
        tall = cells_ref[pl.ds(c * levels, levels), :].T
        anom_out[:, c, :] = tall[:members]
        mean_out[pl.ds(c, 1), :] = tall[members:members + 1]


def near_local(anomalies, state_mean, obs_value, obs_cell, owner, order, root_inv, gain_inv):
    members, lon_dev, lat_dev, levels = anomalies.shape
    classes = lon_dev * lat_dev
    cells = classes * levels
    batches, quarter = obs_value.shape
    obs = obs_cell.shape[1]
    half = obs // 2
    slabs, bands = lax.axis_size("gx"), lax.axis_size("gy")
    piece = quarter // slabs
    early = min(EARLY, batches)
    lat_total = float(bands * lat_dev)
    state, packed, table = pl.pallas_call(
        functools.partial(arrange_kernel, lon_dev, lat_dev, lat_total),
        out_shape=(
            jax.ShapeDtypeStruct((cells, LANES), F32),
            jax.ShapeDtypeStruct((slabs, batches * piece, LANES), F32),
            jax.ShapeDtypeStruct((batches, 2, 2, quarter, half), F32),
        ),
        in_specs=[SMEM] * 4 + [VMEM] * 4,
        out_specs=(VMEM, VMEM, VMEM),
        name="arrange",
    )(
        obs_cell, obs_value, owner, order,
        anomalies.reshape(members, classes, levels), state_mean.reshape(classes, levels), root_inv, gain_inv,
    )

    sizes = (
        members, lon_dev, lat_dev, levels, float(slabs * lon_dev), lat_total, REACH * lon_dev + 1.0, bands, slabs, early
    )
    dma = pltpu.SemaphoreType.DMA
    cells_out = pl.pallas_call(
        functools.partial(analysis_kernel, sizes),
        out_shape=jax.ShapeDtypeStruct((cells, LANES), F32),
        in_specs=[SMEM] * 2 + [VMEM] * 4,
        out_specs=VMEM,
        scratch_shapes=[
            pltpu.VMEM((batches + early, 1, obs), F32),
            pltpu.VMEM((batches + early, 1, obs), F32),
            pltpu.VMEM((slabs, batches * piece, LANES), F32),
            pltpu.VMEM((batches * piece, LANES), F32),
            pltpu.VMEM((batches, piece, LANES), F32),
            pltpu.VMEM((batches + 2, obs, LANES), F32),
            pltpu.VMEM((batches, 2, 2, obs, half), F32),
            pltpu.VMEM((2, 2, 2 * obs, half), BF16),
            pltpu.VMEM((2, 2, 2 * obs, half), BF16),
            pltpu.VMEM((batches + early, 2 * LANES, obs), BF16),
            pltpu.VMEM((batches + early, obs, 2 * LANES), BF16),
            dma((2, slabs)), dma((2, slabs)),
            dma((batches,)), dma((batches,)),
            dma((batches, 2)), dma((batches, 2)),
            dma((batches,)), dma((batches,)),
            dma((batches,)), dma((batches,)),
            dma((batches,)), dma((batches,)),
            dma,
        ],
        compiler_params=pltpu.CompilerParams(collective_id=0, has_side_effects=True),
        name="analysis",
    )(order, owner, state, packed, table, obs_cell)

    post, mean = pl.pallas_call(
        finish_kernel,
        out_shape=(
            jax.ShapeDtypeStruct((members, classes, levels), F32),
            jax.ShapeDtypeStruct((classes, levels), F32),
        ),
        in_specs=[VMEM],
        out_specs=(VMEM, VMEM),
        name="finish",
    )(cells_out)
    return post.reshape(members, lon_dev, lat_dev, levels), mean.reshape(lon_dev, lat_dev, levels)


def local(*arrays):
    obs_value, obs_cell = arrays[2], arrays[3]
    slabs, bands = lax.axis_size("gx"), lax.axis_size("gy")
    piece = obs_value.shape[1] // slabs
    fits = bands == 4 and piece % 8 == 0 and piece * slabs == obs_value.shape[1] and obs_cell.shape[1] == 2 * LANES
    return (near_local if fits and arrays[0].shape[1] == 2 else wide_local)(*arrays)


def solution(mesh):
    return jax.shard_map(
        local,
        mesh=mesh,
        in_specs=(
            P(None, "gx", "gy", None),
            P("gx", "gy", None),
            P(None, "gy"),
            P(),
            P(),
            P(),
            P(None, "gy", None),
            P(None, "gy", None),
        ),
        out_specs=(P(None, "gx", "gy", None), P("gx", "gy", None)),
        check_vma=False,
    )
```

```python
import functools

import jax
import jax.numpy as jnp
from jax import lax
from jax.experimental import pallas as pl
from jax.experimental.pallas import tpu as pltpu
from jax.sharding import PartitionSpec as P

REACH = 3
EARLY = 5
LANES = 128
MESH = pl.DeviceIdType.MESH
VMEM = pl.BlockSpec(memory_space=pltpu.VMEM)
SMEM = pl.BlockSpec(memory_space=pltpu.SMEM)
F32 = jnp.float32
BF16 = jnp.bfloat16


def split(value):
    high = value.astype(BF16)
    return high, (value - high.astype(F32)).astype(BF16)


def nn(left, right):
    return lax.dot_general(left, right, (((1,), (0,)), ((), ())), preferred_element_type=F32)


def nt(left, right):
    return lax.dot_general(left, right, (((1,), (1,)), ((), ())), preferred_element_type=F32)


def lane_ids(shape):
    return lax.broadcasted_iota(jnp.int32, shape, len(shape) - 1)


def pick_kernel(lon_dev, lat_dev, cells_ref, value_ref, owner_ref, order_ref, anom_ref, mean_ref, state_ref, packed_ref, rows_ref):
    column, band = lax.axis_index("gx"), lax.axis_index("gy")
    members, classes, levels = anom_ref.shape
    batches, quarter = value_ref.shape

    for c in range(classes):
        lat = (band * lat_dev + c % lat_dev).astype(F32)
        lon = (column * lon_dev + c // lat_dev).astype(F32)
        tall = jnp.concatenate(
            [
                anom_ref[:, c, :],
                mean_ref[pl.ds(c, 1), :],
                jnp.full((1, levels), lat, F32),
                jnp.full((1, levels), lon, F32),
                jnp.zeros((LANES - members - 3, levels), F32),
            ],
            axis=0,
        )
        state_ref[pl.ds(c * levels, levels), :] = tall.T

    lane = lane_ids((1, LANES))

    def batch(t, _):
        b = order_ref[t]
        mine = owner_ref[b] == column

        @pl.when(mine)
        def _():
            def group(i, _):
                for k in range(8):
                    j = i * 8 + k
                    row = state_ref[pl.ds(cells_ref[b, band * quarter + j], 1), :]
                    rows_ref[pl.ds(t * quarter + j, 1), :] = jnp.where(lane == members + 3, value_ref[b, j], row)
                return 0

            lax.fori_loop(0, quarter // 8, group, 0)

        @pl.when(jnp.logical_not(mine))
        def _():
            rows_ref[pl.ds(pl.multiple_of(t * quarter, quarter), quarter), :] = jnp.zeros((quarter, LANES), F32)

        return 0

    lax.fori_loop(0, batches, batch, 0)
    slabs, height, chunk = packed_ref.shape
    for q in range(slabs):
        packed_ref[q] = rows_ref[pl.ds(q * chunk, chunk), :].T[:height]


def spread_kernel(bands, slabs, rows_ref, out_ref, land, send1, recv1, send2, recv2, send3, recv3, send4, recv4, send5, recv5):
    x, b = lax.axis_index("gx"), lax.axis_index("gy")
    partner = b + 1 - 2 * lax.rem(b, 2)
    across = lax.rem(b + 2, bands)

    def slab(k):
        return lax.rem(x + k, slabs)

    def source(k):
        return lax.rem(x + slabs - k, slabs)

    def first(k):
        return pltpu.make_async_remote_copy(
            src_ref=rows_ref.at[slab(k)], dst_ref=land.at[k], send_sem=send1.at[k], recv_sem=recv1.at[k],
            device_id={"gx": slab(k)}, device_id_type=MESH,
        )

    def second(k):
        return pltpu.make_async_remote_copy(
            src_ref=out_ref.at[b, x], dst_ref=out_ref.at[b, x], send_sem=send2.at[k],
            recv_sem=recv2.at[k], device_id={"gx": slab(k)}, device_id_type=MESH,
        )

    def hand(k, of_band, send_sem, recv_sem, target):
        place = out_ref.at[of_band, source(k)]
        return pltpu.make_async_remote_copy(
            src_ref=place, dst_ref=place, send_sem=send_sem.at[k], recv_sem=recv_sem.at[k],
            device_id={"gy": target}, device_id_type=MESH,
        )

    def third(k):
        return hand(k, b, send3, recv3, partner)

    def fourth(k):
        return hand(k, b, send4, recv4, across)

    def fifth(k):
        return hand(k, across, send5, recv5, partner)

    def each(low, high, body):
        def step(k, _):
            body(k)
            return 0

        lax.fori_loop(low, high, step, 0)

    barrier = pltpu.get_barrier_semaphore()
    each(1, slabs, lambda k: pl.semaphore_signal(barrier, inc=1, device_id={"gx": slab(k)}, device_id_type=MESH))
    for target in (partner, across):
        pl.semaphore_signal(barrier, inc=1, device_id={"gy": target}, device_id_type=MESH)
    pl.semaphore_wait(barrier, slabs + 1)

    each(1, slabs, lambda k: first(k).start())
    out_ref[b, x] = rows_ref[x]

    def add(k):
        first(k).wait_recv()
        out_ref[b, x] += land[k]

    each(1, slabs, add)
    fourth(0).start()
    each(1, slabs, lambda k: second(k).start())
    third(0).start()

    def relay(k):
        second(k).wait_recv()
        fourth(k).start()
        third(k).start()
        fourth(k - 1).wait_recv()
        fifth(k - 1).start()

    each(1, slabs, relay)
    fourth(slabs - 1).wait_recv()
    fifth(slabs - 1).start()

    def finish(k):
        third(k).wait()
        fifth(k).wait()
        fourth(k).wait_send()

    each(0, slabs, finish)

    def sent(k):
        first(k).wait_send()
        second(k).wait_send()

    each(1, slabs, sent)


def main_kernel(
    sizes, order_ref, owner_ref, state_ref, obs_ref, cell_ref, root_ref, gain_ref,
    anom_out, mean_out,
    lat_ref, lon_ref, cells_s, obs_s, v_s, vw_s, z3_s, gh_s, gl_s, send_sem, recv_sem,
):
    members, lon_dev, lat_dev, levels, lon_total, lat_total, span, bands = sizes
    batches, obs = cell_ref.shape
    quarter = obs // bands
    column, band = lax.axis_index("gx"), lax.axis_index("gy")
    classes = lon_dev * lat_dev
    chunk = 4

    barrier = pltpu.get_barrier_semaphore()
    for k in range(1, bands):
        pl.semaphore_signal(barrier, inc=1, device_id={"gy": lax.rem(band + k, bands)}, device_id_type=MESH)
    pl.semaphore_wait(barrier, bands - 1)

    def widen(value, with_low_in_middle):
        high, low = split(value)
        high, low = high.astype(F32), low.astype(F32)
        second, third = (low, high) if with_low_in_middle else (high, low)
        lane = lane_ids(value.shape)
        room = LANES - members
        moved = pltpu.roll(second, members, 1)
        first = jnp.where(lane < members, high, moved)
        last = jnp.where(lane < members - room, moved, pltpu.roll(third, members - room, 1))
        return jnp.concatenate([first, last], axis=1), lane, room

    def state_wide(value):
        return widen(value, True)[0].astype(BF16)

    def prior_wide(value):
        wide, lane, room = widen(jnp.where(lane_ids(value.shape) < members, value, 0.0), False)
        wide_lane = lane_ids(wide.shape)
        return jnp.where(wide_lane < 3 * members, wide, 0.0).astype(BF16)

    def lon_weight(gap):
        gap = jnp.abs(gap)
        gap = jnp.minimum(gap, lon_total - gap)
        return jnp.maximum(0.0, 1.0 - gap * (1.0 / span))

    def lat_weight(gap):
        return 1.0 - jnp.abs(gap) * (1.0 / lat_total)

    def obs_taper(rows, s):
        lat, lon = rows[:, members + 1:members + 2], rows[:, members + 2:members + 3]
        return lat_weight(lat - lat_ref[s]) * lon_weight(lon - lon_ref[s])

    def apply(rows, high, low):
        both = nn(high, vw_s[...])
        return rows - (both[:, :LANES] + both[:, LANES:] + nn(low, vw_s[:, :LANES]))

    def update(rows, taper, s, slot):
        gained = nt(state_wide(rows), z3_s[slot]) * taper
        return apply(rows, *split(gained))

    def update_cells(s, slot):
        for i in range(classes // chunk):
            tapers = []
            for k in range(chunk):
                c = i * chunk + k
                lat = (band * lat_dev + c % lat_dev).astype(F32)
                lon = (column * lon_dev + c // lat_dev).astype(F32)
                weight = lat_weight(lat - lat_ref[s]) * lon_weight(lon - lon_ref[s])
                tapers.append(jnp.broadcast_to(weight, (levels, obs)))
            here = pl.ds(i * chunk * levels, chunk * levels)
            cells_s[here, :] = update(cells_s[here, :], jnp.concatenate(tapers, axis=0), s, slot)

    def at(t):
        return pl.ds(pl.multiple_of(t * obs, obs), obs)

    cells_s[...] = state_ref[...]
    _, slabs, height, width = obs_ref.shape
    part = min(width, quarter)
    for q in range(bands):
        for p in range(slabs):
            rest = jnp.zeros((LANES - height, width), F32)
            block = jnp.concatenate([obs_ref[q, p], rest], axis=0).T
            for i in range(0, width, part):
                t, j = divmod(p * width + i, quarter)
                obs_s[pl.ds(t * obs + q * quarter + j, part), :] = block[i:i + part]
    obs_s[pl.ds(batches * obs, 2 * obs), :] = jnp.zeros((2 * obs, LANES), F32)
    vw_s[...] = jnp.zeros_like(vw_s)
    z3_s[...] = jnp.zeros_like(z3_s)
    first_lat = lax.broadcasted_iota(jnp.int32, (1, obs), 1).astype(F32)
    first_lat = jnp.floor((first_lat + 0.5) * (1.0 / quarter)) * lat_dev
    for t in range(batches):
        batch_id = order_ref[t]
        level_row = jnp.floor((cell_ref[pl.ds(batch_id, 1), :].astype(F32) + 0.5) * (1.0 / levels))
        lon_row = jnp.floor((level_row + 0.5) * (1.0 / lat_dev))
        lat_ref[t] = level_row - lon_row * lat_dev + first_lat
        lon_ref[t] = lon_row + (owner_ref[batch_id] * lon_dev).astype(F32)

    def turn(t, _):
        prior = obs_s[at(t), :]
        lane = lane_ids(prior.shape)
        innovation = pltpu.roll(prior, LANES - 3, 1) - prior
        joined = jnp.where(lane < members, prior, jnp.where(lane == members, innovation, 0.0))
        high, low = split(joined)
        batch_id = order_ref[t]
        table_high, table_low = split(jnp.concatenate([root_ref[batch_id], gain_ref[batch_id]], axis=0))
        both = nn(table_high, jnp.concatenate([high, low], axis=1))
        part = both[:, :LANES] + both[:, LANES:] + nn(table_low, high)
        lane = lane_ids((quarter, LANES))
        weighted = jnp.where(lane < members, part[:quarter], jnp.where(lane == members, -part[quarter:], 0.0))
        mine = pl.ds(pl.multiple_of(band * quarter, quarter), quarter)
        v_s[t, mine, :] = weighted * (1.0 / (members - 1.0))

        def copy(k):
            return pltpu.make_async_remote_copy(
                src_ref=v_s.at[t, mine, :],
                dst_ref=v_s.at[t, mine, :],
                send_sem=send_sem.at[t, k - 1],
                recv_sem=recv_sem.at[t, k - 1],
                device_id={"gy": lax.rem(band + k, bands)},
                device_id_type=MESH,
            )

        for k in range(1, bands):
            copy(k).start()

        z3_s[lax.rem(t, 2)] = prior_wide(prior)

        before = jnp.maximum(t - 1, 0)
        past = lax.rem(t + 1, 2)
        rows = obs_s[at(t + 1), :]
        rows = update(rows, obs_taper(rows, before), before, past)
        obs_s[at(t + 1), :] = rows
        gained = nt(state_wide(rows), z3_s[lax.rem(t, 2)]) * obs_taper(rows, t)
        gh_s[...], gl_s[...] = split(gained)
        update_cells(before, past)

        def later(i, _):
            here = pl.ds(pl.multiple_of((t + 2 + 2 * i) * obs, obs), 2 * obs)
            rows = obs_s[here, :]
            obs_s[here, :] = update(rows, obs_taper(rows, before), before, past)
            return 0

        lax.fori_loop(0, (batches - 1 - t) // 2 * jnp.minimum(t, 1), later, 0)

        for k in range(1, bands):
            copy(k).wait()

        vw_s[...] = jnp.concatenate(split(v_s[t]), axis=1)

        obs_s[at(t + 1), :] = apply(obs_s[at(t + 1), :], gh_s[...], gl_s[...])
        return 0

    lax.fori_loop(0, batches, turn, 0)
    update_cells(batches - 1, (batches - 1) % 2)
    for c in range(classes):
        tall = cells_s[pl.ds(c * levels, levels), :].T
        anom_out[:, c, :] = tall[:members]
        mean_out[pl.ds(c, 1), :] = tall[members:members + 1]


def wide_local(anomalies, state_mean, obs_value, obs_cell, owner, order, root_inv, gain_inv):
    members, lon_dev, lat_dev, levels = anomalies.shape
    classes = lon_dev * lat_dev
    cells = classes * levels
    batches, quarter = obs_value.shape
    obs = obs_cell.shape[1]
    slabs, bands = lax.axis_size("gx"), lax.axis_size("gy")
    chunk = batches * quarter // slabs
    height = (members + 4 + 7) // 8 * 8
    state, rows = pl.pallas_call(
        functools.partial(pick_kernel, lon_dev, lat_dev),
        out_shape=(
            jax.ShapeDtypeStruct((cells, LANES), F32),
            jax.ShapeDtypeStruct((slabs, height, chunk), F32),
        ),
        in_specs=[SMEM] * 4 + [VMEM] * 2,
        out_specs=(VMEM, VMEM),
        scratch_shapes=[pltpu.VMEM((batches * quarter, LANES), F32)],
        name="pick",
    )(
        obs_cell, obs_value, owner, order,
        anomalies.reshape(members, classes, levels), state_mean.reshape(classes, levels),
    )

    rows = pl.pallas_call(
        functools.partial(spread_kernel, bands, slabs),
        out_shape=jax.ShapeDtypeStruct((bands, slabs, height, chunk), F32),
        in_specs=[VMEM],
        out_specs=VMEM,
        scratch_shapes=[pltpu.VMEM((slabs, height, chunk), F32)] + [pltpu.SemaphoreType.DMA((slabs,))] * 10,
        compiler_params=pltpu.CompilerParams(collective_id=1, has_side_effects=True),
        name="spread",
    )(rows)

    sizes = (
        members, lon_dev, lat_dev, levels, float(slabs * lon_dev), float(bands * lat_dev), REACH * lon_dev + 1.0, bands
    )
    post, mean = pl.pallas_call(
        functools.partial(main_kernel, sizes),
        out_shape=(
            jax.ShapeDtypeStruct((members, classes, levels), F32),
            jax.ShapeDtypeStruct((classes, levels), F32),
        ),
        in_specs=[SMEM] * 2 + [VMEM] * 5,
        out_specs=(VMEM, VMEM),
        scratch_shapes=[
            pltpu.VMEM((batches, 1, obs), F32),
            pltpu.VMEM((batches, 1, obs), F32),
            pltpu.VMEM((cells, LANES), F32),
            pltpu.VMEM(((batches + 2) * obs, LANES), F32),
            pltpu.VMEM((batches, obs, LANES), F32),
            pltpu.VMEM((obs, 2 * LANES), BF16),
            pltpu.VMEM((2, obs, 2 * LANES), BF16),
            pltpu.VMEM((obs, obs), BF16),
            pltpu.VMEM((obs, obs), BF16),
            pltpu.SemaphoreType.DMA((batches, bands - 1)),
            pltpu.SemaphoreType.DMA((batches, bands - 1)),
        ],
        compiler_params=pltpu.CompilerParams(collective_id=0, has_side_effects=True),
        name="analysis",
    )(
        order, owner, state, rows, obs_cell, root_inv, gain_inv,
    )
    return post.reshape(members, lon_dev, lat_dev, levels), mean.reshape(lon_dev, lat_dev, levels)


def analysis_kernel(
    sizes, index_ref, order_ref, owner_ref, cell_ref, value_ref, anom_ref, mean_ref, root_ref, gain_ref,
    cells_s,
    lat_ref, lon_ref, pick_s, packed_s, land, mine_s, share_s, obs_s, full_s, th_s, tl_s, z3_s, vw_s,
    rs_send, rs_recv, send1, recv1, send2, recv2, send3, recv3, near_send, near_recv, far_send, far_recv, hand_send, hand_recv,
):
    members, lon_dev, lat_dev, levels, lon_total, lat_total, span, bands, slabs, early = sizes
    batches, obs = cell_ref.shape
    quarter, half = obs // bands, obs // 2
    piece = quarter // slabs
    ahead = min(5, batches)
    column, band = lax.axis_index("gx"), lax.axis_index("gy")
    partner = band + 1 - 2 * lax.rem(band, 2)
    across = lax.rem(band + bands // 2, bands)
    near = lax.div(band, bands // 2)
    far = 1 - near
    classes = lon_dev * lat_dev
    chunk = 4

    def slab(k):
        return lax.rem(column + k, slabs)

    def band_rows(b):
        return pl.ds(pl.multiple_of(b * quarter, quarter), quarter)

    def half_rows(h):
        return pl.ds(pl.multiple_of(h * half, half), half)

    def remote(src, dst, send, recv, device):
        return pltpu.make_async_remote_copy(
            src_ref=src, dst_ref=dst, send_sem=send, recv_sem=recv, device_id=device, device_id_type=MESH
        )

    ends = (0, 3, early + 2, batches)

    def part_rows(p):
        return pl.ds(ends[p] * piece, (ends[p + 1] - ends[p]) * piece)

    def reduce_copy(k, p):
        here = part_rows(p)
        return remote(
            packed_s.at[slab(k), here], land.at[k, here], rs_send.at[p, k], rs_recv.at[p, k], {"gx": slab(k)}
        )

    def my_piece(s):
        return pl.ds(pl.multiple_of(s * piece, piece), piece)

    rank, side = lax.div(column, 2), lax.rem(column, 2)
    ranks = slabs // 2

    def keep(s):
        rows = mine_s[my_piece(s), :]
        share_s[s] = rows
        obs_s[s, band, rank, side] = rows

        def start(device):
            remote(share_s.at[s], obs_s.at[s, band, rank, side], send1.at[s], recv1.at[s], device).start()

        return start

    def share_ranks(s):
        start = keep(s)
        for k in range(1, ranks):
            start({"gx": 2 * lax.rem(rank + k, ranks) + side})

    def share_sides(s):
        pieces(s, ranks - 1, recv1)
        place = obs_s.at[s, band, :, side]
        for target in ({"gx": 2 * rank + 1 - side}, {"gy": across}, {"gx": 2 * rank + 1 - side, "gy": across}):
            remote(place, place, send3.at[s], recv3.at[s], target).start()

    def share(s):
        start = keep(s)

        for k in range(1, slabs):
            start({"gx": slab(k)})
        for k in range(slabs):
            start({"gx": slab(k), "gy": across})

    def pieces(s, count, sem):
        window = mine_s.at[pl.ds(0, count * piece)]
        pltpu.make_async_copy(window, window, sem.at[s]).wait()

    def shared(s, sem):
        pieces(s, 2 * slabs - 1, sem)

    def pass_on(s, i):
        place = obs_s.at[s, (band, across)[i]]
        return remote(place, place, send2.at[s, i], recv2.at[s, i], {"gy": partner})

    def near_copy(t):
        return remote(
            full_s.at[t, :, :, band_rows(band)], full_s.at[t, :, :, band_rows(band)], near_send.at[t], near_recv.at[t], {"gy": partner}
        )

    def far_copy(t):
        return remote(
            full_s.at[t, :, near, band_rows(band)], full_s.at[t, :, near, band_rows(band)], far_send.at[t],
            far_recv.at[t], {"gy": across},
        )

    def hand_copy(t):
        place = full_s.at[t, :, far, band_rows(across)]
        return remote(place, place, hand_send.at[t], hand_recv.at[t], {"gy": partner})

    def send_table(t):
        far_copy(t).start()
        near_copy(t).start()

    def hand_table(t):
        far_copy(t).wait_recv()
        hand_copy(t).start()

    def prepare(t, slot):
        for k in range(2):
            aside = full_s[t, k, far, half_rows(near), :]
            blocks = (
                (near, near, full_s[t, k, near, half_rows(near), :]),
                (far, near, aside),
                (near, far, aside.T),
                (far, far, full_s[t, k, far, half_rows(far), :]),
            )
            for columns, rows, block in blocks:
                here = pl.ds(pl.multiple_of(k * obs + rows * half, half), half)
                high, low = split(block)
                th_s[slot, columns, here, :] = high
                tl_s[slot, columns, here, :] = low

    barrier = pltpu.get_barrier_semaphore()
    for k in range(1, slabs):
        pl.semaphore_signal(barrier, inc=1, device_id={"gx": slab(k)}, device_id_type=MESH)
    for k in range(slabs):
        pl.semaphore_signal(barrier, inc=1, device_id={"gx": slab(k), "gy": across}, device_id_type=MESH)
    pl.semaphore_signal(barrier, inc=1, device_id={"gy": partner}, device_id_type=MESH)

    for c in range(classes):
        lat = (band * lat_dev + c % lat_dev).astype(F32) * (1.0 / lat_total)
        lon = (column * lon_dev + c // lat_dev).astype(F32)
        tall = jnp.concatenate(
            [
                anom_ref[:, c, :],
                mean_ref[pl.ds(c, 1), :],
                jnp.full((1, levels), lat, F32),
                jnp.full((1, levels), lon, F32),
                jnp.zeros((1, levels), F32),
                jnp.full((1, levels), float(c // lat_dev), F32),
                jnp.zeros((LANES - members - 5, levels), F32),
            ],
            axis=0,
        )
        cells_s[pl.ds(c * levels, levels), :] = tall.T

    def pick(t, _):
        b = order_ref[t]
        for j in range(quarter):
            pick_s[pl.ds(j, 1), :] = cells_s[pl.ds(index_ref[b, band * quarter + j], 1), :]
        block = pick_s[...]
        values = jnp.broadcast_to(value_ref[pl.ds(b, 1), :], (LANES, quarter)).T
        block = jnp.where(lane_ids(block.shape) == members + 3, values, block)
        block = jnp.where(owner_ref[b] == column, block, 0.0)
        packed_s[:, my_piece(t), :] = block.reshape(slabs, piece, LANES)
        return 0

    def spread_part(p):
        for k in range(1, slabs):
            reduce_copy(k, p).start()

    def stage(t, _):
        b = order_ref[t]
        for h in range(2):
            full_s[t, 0, h, band_rows(band), :] = root_ref[b, :, h * half:(h + 1) * half]
            full_s[t, 1, h, band_rows(band), :] = gain_ref[b, :, h * half:(h + 1) * half]
        return 0

    lax.fori_loop(ends[0], ends[1], pick, 0)
    pl.semaphore_wait(barrier, 2 * slabs)
    spread_part(0)
    stage(0, 0)
    send_table(0)
    lax.fori_loop(ends[1], ends[2], pick, 0)
    spread_part(1)
    lax.fori_loop(1, batches, stage, 0)
    lax.fori_loop(ends[2], ends[3], pick, 0)

    first_lat = lax.broadcasted_iota(jnp.int32, (1, obs), 1).astype(F32)
    first_lat = jnp.floor((first_lat + 0.5) * (1.0 / quarter)) * lat_dev
    for t in range(batches):
        batch_id = order_ref[t]
        level_row = jnp.floor((cell_ref[pl.ds(batch_id, 1), :].astype(F32) + 0.5) * (1.0 / levels))
        lon_row = jnp.floor((level_row + 0.5) * (1.0 / lat_dev))
        lat_ref[t + early] = (level_row - lon_row * lat_dev + first_lat) * (1.0 / lat_total)
        lon_ref[t + early] = lon_row + (owner_ref[batch_id] * lon_dev).astype(F32)
    for t in range(early):
        lat_ref[t] = jnp.zeros((1, obs), F32)
        lon_ref[t] = jnp.zeros((1, obs), F32)
        vw_s[t] = jnp.zeros(vw_s.shape[1:], BF16)
        z3_s[t] = jnp.zeros(z3_s.shape[1:], BF16)
    for s in range(batches, obs_s.shape[0]):
        obs_s[s] = jnp.zeros(obs_s.shape[1:], F32)
    mine_s[...] = jnp.zeros_like(mine_s)

    def collect(p):
        here = part_rows(p)
        total = packed_s[column, here, :]
        for k in range(1, slabs):
            reduce_copy(k, p).wait_recv()
            total = total + land[k, here, :]
        return total

    mine_s[part_rows(0), :] = collect(0)
    for s in range(ends[1]):
        share_ranks(s)
    mine_s[part_rows(1), :] = collect(1)
    for s in range(ends[1], early):
        share(s)
    spread_part(2)
    for s in range(ends[1]):
        share_sides(s)
    for t in range(1, ahead):
        send_table(t)
    hand_table(0)
    near_copy(0).wait_recv()
    hand_copy(0).wait_recv()
    prepare(0, 0)

    def pass_both(s):
        for i in range(2):
            pass_on(s, i).start()

    def passed(s):
        for i in range(2):
            pass_on(s, i).wait()

    for s in range(2):
        pieces(s, 3 * ranks, recv3)
        pass_both(s)
    for t in range(1, 3):
        hand_table(t)
    for s in range(2):
        passed(s)
    pieces(2, 3 * ranks, recv3)
    for s in range(ends[1]):
        pieces(s, 3 * ranks, send3)

    def state_wide(value):
        low = value - value.astype(BF16).astype(F32)
        lane = lane_ids(value.shape)
        room = LANES - members
        moved = pltpu.roll(low, members, 1)
        first = jnp.where(lane < members, value, moved)
        last = jnp.where(lane < members - room, moved, pltpu.roll(value, members - room, 1))
        return jnp.concatenate([first.astype(BF16), last.astype(BF16)], axis=1)

    def prior_tall(prior):
        high, low = split(prior.T[:members])
        return jnp.concatenate([high, high, low, jnp.zeros((2 * LANES - 3 * members, obs), BF16)], axis=0)

    def lon_weight(gap):
        gap = jnp.abs(gap)
        gap = jnp.minimum(gap, lon_total - gap)
        return jnp.maximum(0.0, 1.0 - gap * (1.0 / span))

    def lat_weight(gap):
        return 1.0 - jnp.abs(gap)

    def apply(rows, high, low, vw):
        both = nn(high, vw)
        return rows - (both[:, :LANES] + both[:, LANES:] + nn(low, vw[:, :LANES]))

    def gain_of(rows, taper, z3):
        return split(nn(state_wide(rows), z3) * taper)

    def update(rows, taper, z3, vw):
        high, low = gain_of(rows, taper, z3)
        return apply(rows, high, low, vw)

    def obs_taper(lat, bit, s, e):
        lon = (owner_ref[order_ref[jnp.minimum(s, batches - 1)]] * lon_dev).astype(F32)
        west = lon_weight(lon - lon_ref[e])
        east = lon_weight(lon + 1.0 - lon_ref[e])
        return lat_weight(lat - lat_ref[e]) * (west + bit * (east - west))

    def update_mine(rows, e, z3, vw):
        lat, lon = rows[:, members + 1:members + 2], rows[:, members + 2:members + 3]
        taper = lat_weight(lat - lat_ref[e]) * lon_weight(lon - lon_ref[e])
        return update(rows, taper, z3, vw)

    def update_cells(e, part):
        tapers = []
        for k in range(chunk):
            c = part * chunk + k
            lat = (band * lat_dev + c % lat_dev).astype(F32) * (1.0 / lat_total)
            lon = (column * lon_dev + c // lat_dev).astype(F32)
            weight = lat_weight(lat - lat_ref[e]) * lon_weight(lon - lon_ref[e])
            tapers.append(jnp.broadcast_to(weight, (levels, obs)))
        here = pl.ds(part * chunk * levels, chunk * levels)
        cells_s[here, :] = update(cells_s[here, :], jnp.concatenate(tapers, axis=0), z3_s[e], vw_s[e])

    cell_parts = classes // chunk

    def turn(t, _):
        slot = lax.rem(t, 2)
        e = t + early

        @pl.when(t == ends[2] - early)
        def _():
            rows = collect(2)
            for k in range(ends[2] - early):
                rows = update_mine(rows, early + k, z3_s[early + k], vw_s[early + k])
            mine_s[part_rows(2), :] = rows

        @pl.when(e < batches)
        def _():
            share(e)

        @pl.when(t + 2 < batches)
        def _():
            pass_both(t + 2)

        @pl.when(t + 3 < batches)
        def _():
            shared(t + 3, recv1)

        @pl.when(t + ahead < batches)
        def _():
            send_table(t + ahead)

        @pl.when(t + 3 < batches)
        def _():
            hand_table(t + 3)

        @pl.when(t + 1 < batches)
        def _():
            near_copy(t + 1).wait_recv()
            hand_copy(t + 1).wait_recv()

        @pl.when(jnp.logical_and(t > 0, t + 1 < batches))
        def _():
            passed(t + 1)

        prior = obs_s[t].reshape(obs, LANES)
        rows = obs_s[t + 1].reshape(obs, LANES)
        coming = t + 3
        later = jnp.concatenate(
            [obs_s[coming, place].reshape(quarter, LANES) for place in (band, across)], axis=0
        )
        lat, bit = rows[:, members + 1:members + 2], rows[:, members + 4:members + 5]
        later_lat, later_bit = later[:, members + 1:members + 2], later[:, members + 4:members + 5]
        done = 0

        def some_cells(upto):
            nonlocal done
            while done < min(upto, cell_parts):
                update_cells(e - 1, done)
                done += 1

        def catch_up(later, k, z3, vw):
            return update(later, obs_taper(later_lat, later_bit, coming, e - k), z3, vw)

        lane = lane_ids(prior.shape)
        innovation = pltpu.roll(prior, LANES - 3, 1) - prior
        joined = jnp.where(lane < members, prior, jnp.where(lane == members, innovation, 0.0))
        high, low = split(joined)
        table_high = jnp.concatenate([th_s[slot, 0], th_s[slot, 1]], axis=1)
        table_low = jnp.concatenate([tl_s[slot, 0], tl_s[slot, 1]], axis=1)
        both = nn(table_high, jnp.concatenate([high, low], axis=1))
        part = both[:, :LANES] + both[:, LANES:] + nn(table_low, high)
        lane = lane_ids((obs, LANES))
        weighted = jnp.where(lane < members, part[:obs], jnp.where(lane == members, -part[obs:], 0.0))
        vw = jnp.concatenate(split(weighted * (1.0 / (members - 1.0))), axis=1)
        z3 = prior_tall(prior)

        later = catch_up(later, 2, z3_s[e - 2], vw_s[e - 2])
        rows = update(rows, obs_taper(lat, bit, t + 1, e - 1), z3_s[e - 1], vw_s[e - 1])
        some_cells(1)
        gained = gain_of(rows, obs_taper(lat, bit, t + 1, e), z3)
        later = catch_up(later, 1, z3_s[e - 1], vw_s[e - 1])
        some_cells(2)
        obs_s[t + 1] = apply(rows, *gained, vw).reshape(obs_s.shape[1:])
        some_cells(3)
        later = catch_up(later, 0, z3, vw)
        for i, place in enumerate((band, across)):
            obs_s[coming, place] = later[i * quarter:(i + 1) * quarter].reshape(obs_s.shape[2:])
        mine_s[...] = update_mine(mine_s[...], e, z3, vw)
        some_cells(cell_parts)
        z3_s[e] = z3
        vw_s[e] = vw
        prepare(jnp.minimum(t + 1, batches - 1), 1 - slot)
        return 0

    lax.fori_loop(0, batches, turn, 0)
    for i in range(cell_parts):
        update_cells(batches - 1 + early, i)

    for p in range(3):
        for k in range(1, slabs):
            reduce_copy(k, p).wait_send()

    def sent(t, _):
        near_copy(t).wait_send()
        far_copy(t).wait_send()
        hand_copy(t).wait_send()
        return 0

    lax.fori_loop(0, batches, sent, 0)
    for s in range(ends[1]):
        pieces(s, ranks - 1, send1)

    def shared_sent(s, _):
        shared(s, send1)
        return 0

    lax.fori_loop(ends[1], batches, shared_sent, 0)


def finish_kernel(cells_ref, anom_out, mean_out):
    members, classes, levels = anom_out.shape
    for c in range(classes):
        tall = cells_ref[pl.ds(c * levels, levels), :].T
        anom_out[:, c, :] = tall[:members]
        mean_out[pl.ds(c, 1), :] = tall[members:members + 1]


def near_local(anomalies, state_mean, obs_value, obs_cell, owner, order, root_inv, gain_inv):
    members, lon_dev, lat_dev, levels = anomalies.shape
    classes = lon_dev * lat_dev
    cells = classes * levels
    batches, quarter = obs_value.shape
    obs = obs_cell.shape[1]
    half = obs // 2
    slabs, bands = lax.axis_size("gx"), lax.axis_size("gy")
    piece = quarter // slabs
    early = min(EARLY, batches)
    lat_total = float(bands * lat_dev)
    sizes = (
        members, lon_dev, lat_dev, levels, float(slabs * lon_dev), lat_total, REACH * lon_dev + 1.0, bands, slabs, early
    )
    dma = pltpu.SemaphoreType.DMA
    cells_out = pl.pallas_call(
        functools.partial(analysis_kernel, sizes),
        out_shape=jax.ShapeDtypeStruct((cells, LANES), F32),
        in_specs=[SMEM] * 3 + [VMEM] * 6,
        out_specs=VMEM,
        scratch_shapes=[
            pltpu.VMEM((batches + early, 1, obs), F32),
            pltpu.VMEM((batches + early, 1, obs), F32),
            pltpu.VMEM((quarter, LANES), F32),
            pltpu.VMEM((slabs, batches * piece, LANES), F32),
            pltpu.VMEM((slabs, batches * piece, LANES), F32),
            pltpu.VMEM((batches * piece, LANES), F32),
            pltpu.VMEM((batches, piece, LANES), F32),
            pltpu.VMEM((batches + 3, bands, slabs // 2, 2, piece, LANES), F32),
            pltpu.VMEM((batches, 2, 2, obs, half), F32),
            pltpu.VMEM((2, 2, 2 * obs, half), BF16),
            pltpu.VMEM((2, 2, 2 * obs, half), BF16),
            pltpu.VMEM((batches + early, 2 * LANES, obs), BF16),
            pltpu.VMEM((batches + early, obs, 2 * LANES), BF16),
            dma((3, slabs)), dma((3, slabs)),
            dma((batches,)), dma((batches,)),
            dma((batches, 2)), dma((batches, 2)),
            dma((3,)), dma((3,)),
            dma((batches,)), dma((batches,)),
            dma((batches,)), dma((batches,)),
            dma((batches,)), dma((batches,)),
        ],
        compiler_params=pltpu.CompilerParams(collective_id=0, has_side_effects=True),
        name="analysis",
    )(
        obs_cell, order, owner, obs_cell, obs_value,
        anomalies.reshape(members, classes, levels), state_mean.reshape(classes, levels), root_inv, gain_inv,
    )

    post, mean = pl.pallas_call(
        finish_kernel,
        out_shape=(
            jax.ShapeDtypeStruct((members, classes, levels), F32),
            jax.ShapeDtypeStruct((classes, levels), F32),
        ),
        in_specs=[VMEM],
        out_specs=(VMEM, VMEM),
        name="finish",
    )(cells_out)
    return post.reshape(members, lon_dev, lat_dev, levels), mean.reshape(lon_dev, lat_dev, levels)


def local(*arrays):
    obs_value, obs_cell = arrays[2], arrays[3]
    slabs, bands = lax.axis_size("gx"), lax.axis_size("gy")
    piece = obs_value.shape[1] // slabs
    fits = bands == 4 and piece % 8 == 0 and piece * slabs == obs_value.shape[1] and obs_cell.shape[1] == 2 * LANES
    return (near_local if fits and arrays[0].shape[1] == 2 else wide_local)(*arrays)


def solution(mesh):
    return jax.shard_map(
        local,
        mesh=mesh,
        in_specs=(
            P(None, "gx", "gy", None),
            P("gx", "gy", None),
            P(None, "gy"),
            P(),
            P(),
            P(),
            P(None, "gy", None),
            P(None, "gy", None),
        ),
        out_specs=(P(None, "gx", "gy", None), P("gx", "gy", None)),
        check_vma=False,
    )
```

```python
import functools

import jax
import jax.numpy as jnp
from jax import lax
from jax.experimental import pallas as pl
from jax.experimental.pallas import tpu as pltpu
from jax.sharding import PartitionSpec as P

REACH = 3
EARLY = 5
LANES = 128
MESH = pl.DeviceIdType.MESH
VMEM = pl.BlockSpec(memory_space=pltpu.VMEM)
SMEM = pl.BlockSpec(memory_space=pltpu.SMEM)
F32 = jnp.float32
BF16 = jnp.bfloat16


def split(value):
    high = value.astype(BF16)
    return high, (value - high.astype(F32)).astype(BF16)


def nn(left, right):
    return lax.dot_general(left, right, (((1,), (0,)), ((), ())), preferred_element_type=F32)


def nt(left, right):
    return lax.dot_general(left, right, (((1,), (1,)), ((), ())), preferred_element_type=F32)


def lane_ids(shape):
    return lax.broadcasted_iota(jnp.int32, shape, len(shape) - 1)


def pick_kernel(lon_dev, lat_dev, cells_ref, value_ref, owner_ref, order_ref, anom_ref, mean_ref, state_ref, packed_ref, rows_ref):
    column, band = lax.axis_index("gx"), lax.axis_index("gy")
    members, classes, levels = anom_ref.shape
    batches, quarter = value_ref.shape

    for c in range(classes):
        lat = (band * lat_dev + c % lat_dev).astype(F32)
        lon = (column * lon_dev + c // lat_dev).astype(F32)
        tall = jnp.concatenate(
            [
                anom_ref[:, c, :],
                mean_ref[pl.ds(c, 1), :],
                jnp.full((1, levels), lat, F32),
                jnp.full((1, levels), lon, F32),
                jnp.zeros((LANES - members - 3, levels), F32),
            ],
            axis=0,
        )
        state_ref[pl.ds(c * levels, levels), :] = tall.T

    lane = lane_ids((1, LANES))

    def batch(t, _):
        b = order_ref[t]
        mine = owner_ref[b] == column

        @pl.when(mine)
        def _():
            def group(i, _):
                for k in range(8):
                    j = i * 8 + k
                    row = state_ref[pl.ds(cells_ref[b, band * quarter + j], 1), :]
                    rows_ref[pl.ds(t * quarter + j, 1), :] = jnp.where(lane == members + 3, value_ref[b, j], row)
                return 0

            lax.fori_loop(0, quarter // 8, group, 0)

        @pl.when(jnp.logical_not(mine))
        def _():
            rows_ref[pl.ds(pl.multiple_of(t * quarter, quarter), quarter), :] = jnp.zeros((quarter, LANES), F32)

        return 0

    lax.fori_loop(0, batches, batch, 0)
    slabs, height, chunk = packed_ref.shape
    for q in range(slabs):
        packed_ref[q] = rows_ref[pl.ds(q * chunk, chunk), :].T[:height]


def spread_kernel(bands, slabs, rows_ref, out_ref, land, send1, recv1, send2, recv2, send3, recv3, send4, recv4, send5, recv5):
    x, b = lax.axis_index("gx"), lax.axis_index("gy")
    partner = b + 1 - 2 * lax.rem(b, 2)
    across = lax.rem(b + 2, bands)

    def slab(k):
        return lax.rem(x + k, slabs)

    def source(k):
        return lax.rem(x + slabs - k, slabs)

    def first(k):
        return pltpu.make_async_remote_copy(
            src_ref=rows_ref.at[slab(k)], dst_ref=land.at[k], send_sem=send1.at[k], recv_sem=recv1.at[k],
            device_id={"gx": slab(k)}, device_id_type=MESH,
        )

    def second(k):
        return pltpu.make_async_remote_copy(
            src_ref=out_ref.at[b, x], dst_ref=out_ref.at[b, x], send_sem=send2.at[k],
            recv_sem=recv2.at[k], device_id={"gx": slab(k)}, device_id_type=MESH,
        )

    def hand(k, of_band, send_sem, recv_sem, target):
        place = out_ref.at[of_band, source(k)]
        return pltpu.make_async_remote_copy(
            src_ref=place, dst_ref=place, send_sem=send_sem.at[k], recv_sem=recv_sem.at[k],
            device_id={"gy": target}, device_id_type=MESH,
        )

    def third(k):
        return hand(k, b, send3, recv3, partner)

    def fourth(k):
        return hand(k, b, send4, recv4, across)

    def fifth(k):
        return hand(k, across, send5, recv5, partner)

    def each(low, high, body):
        def step(k, _):
            body(k)
            return 0

        lax.fori_loop(low, high, step, 0)

    barrier = pltpu.get_barrier_semaphore()
    each(1, slabs, lambda k: pl.semaphore_signal(barrier, inc=1, device_id={"gx": slab(k)}, device_id_type=MESH))
    for target in (partner, across):
        pl.semaphore_signal(barrier, inc=1, device_id={"gy": target}, device_id_type=MESH)
    pl.semaphore_wait(barrier, slabs + 1)

    each(1, slabs, lambda k: first(k).start())
    out_ref[b, x] = rows_ref[x]

    def add(k):
        first(k).wait_recv()
        out_ref[b, x] += land[k]

    each(1, slabs, add)
    fourth(0).start()
    each(1, slabs, lambda k: second(k).start())
    third(0).start()

    def relay(k):
        second(k).wait_recv()
        fourth(k).start()
        third(k).start()
        fourth(k - 1).wait_recv()
        fifth(k - 1).start()

    each(1, slabs, relay)
    fourth(slabs - 1).wait_recv()
    fifth(slabs - 1).start()

    def finish(k):
        third(k).wait()
        fifth(k).wait()
        fourth(k).wait_send()

    each(0, slabs, finish)

    def sent(k):
        first(k).wait_send()
        second(k).wait_send()

    each(1, slabs, sent)


def main_kernel(
    sizes, order_ref, owner_ref, state_ref, obs_ref, cell_ref, root_ref, gain_ref,
    anom_out, mean_out,
    lat_ref, lon_ref, cells_s, obs_s, v_s, vw_s, z3_s, gh_s, gl_s, send_sem, recv_sem,
):
    members, lon_dev, lat_dev, levels, lon_total, lat_total, span, bands = sizes
    batches, obs = cell_ref.shape
    quarter = obs // bands
    column, band = lax.axis_index("gx"), lax.axis_index("gy")
    classes = lon_dev * lat_dev
    chunk = 4

    barrier = pltpu.get_barrier_semaphore()
    for k in range(1, bands):
        pl.semaphore_signal(barrier, inc=1, device_id={"gy": lax.rem(band + k, bands)}, device_id_type=MESH)
    pl.semaphore_wait(barrier, bands - 1)

    def widen(value, with_low_in_middle):
        high, low = split(value)
        high, low = high.astype(F32), low.astype(F32)
        second, third = (low, high) if with_low_in_middle else (high, low)
        lane = lane_ids(value.shape)
        room = LANES - members
        moved = pltpu.roll(second, members, 1)
        first = jnp.where(lane < members, high, moved)
        last = jnp.where(lane < members - room, moved, pltpu.roll(third, members - room, 1))
        return jnp.concatenate([first, last], axis=1), lane, room

    def state_wide(value):
        return widen(value, True)[0].astype(BF16)

    def prior_wide(value):
        wide, lane, room = widen(jnp.where(lane_ids(value.shape) < members, value, 0.0), False)
        wide_lane = lane_ids(wide.shape)
        return jnp.where(wide_lane < 3 * members, wide, 0.0).astype(BF16)

    def lon_weight(gap):
        gap = jnp.abs(gap)
        gap = jnp.minimum(gap, lon_total - gap)
        return jnp.maximum(0.0, 1.0 - gap * (1.0 / span))

    def lat_weight(gap):
        return 1.0 - jnp.abs(gap) * (1.0 / lat_total)

    def obs_taper(rows, s):
        lat, lon = rows[:, members + 1:members + 2], rows[:, members + 2:members + 3]
        return lat_weight(lat - lat_ref[s]) * lon_weight(lon - lon_ref[s])

    def apply(rows, high, low):
        both = nn(high, vw_s[...])
        return rows - (both[:, :LANES] + both[:, LANES:] + nn(low, vw_s[:, :LANES]))

    def update(rows, taper, s, slot):
        gained = nt(state_wide(rows), z3_s[slot]) * taper
        return apply(rows, *split(gained))

    def update_cells(s, slot):
        for i in range(classes // chunk):
            tapers = []
            for k in range(chunk):
                c = i * chunk + k
                lat = (band * lat_dev + c % lat_dev).astype(F32)
                lon = (column * lon_dev + c // lat_dev).astype(F32)
                weight = lat_weight(lat - lat_ref[s]) * lon_weight(lon - lon_ref[s])
                tapers.append(jnp.broadcast_to(weight, (levels, obs)))
            here = pl.ds(i * chunk * levels, chunk * levels)
            cells_s[here, :] = update(cells_s[here, :], jnp.concatenate(tapers, axis=0), s, slot)

    def at(t):
        return pl.ds(pl.multiple_of(t * obs, obs), obs)

    cells_s[...] = state_ref[...]
    _, slabs, height, width = obs_ref.shape
    part = min(width, quarter)
    for q in range(bands):
        for p in range(slabs):
            rest = jnp.zeros((LANES - height, width), F32)
            block = jnp.concatenate([obs_ref[q, p], rest], axis=0).T
            for i in range(0, width, part):
                t, j = divmod(p * width + i, quarter)
                obs_s[pl.ds(t * obs + q * quarter + j, part), :] = block[i:i + part]
    obs_s[pl.ds(batches * obs, 2 * obs), :] = jnp.zeros((2 * obs, LANES), F32)
    vw_s[...] = jnp.zeros_like(vw_s)
    z3_s[...] = jnp.zeros_like(z3_s)
    first_lat = lax.broadcasted_iota(jnp.int32, (1, obs), 1).astype(F32)
    first_lat = jnp.floor((first_lat + 0.5) * (1.0 / quarter)) * lat_dev
    for t in range(batches):
        batch_id = order_ref[t]
        level_row = jnp.floor((cell_ref[pl.ds(batch_id, 1), :].astype(F32) + 0.5) * (1.0 / levels))
        lon_row = jnp.floor((level_row + 0.5) * (1.0 / lat_dev))
        lat_ref[t] = level_row - lon_row * lat_dev + first_lat
        lon_ref[t] = lon_row + (owner_ref[batch_id] * lon_dev).astype(F32)

    def turn(t, _):
        prior = obs_s[at(t), :]
        lane = lane_ids(prior.shape)
        innovation = pltpu.roll(prior, LANES - 3, 1) - prior
        joined = jnp.where(lane < members, prior, jnp.where(lane == members, innovation, 0.0))
        high, low = split(joined)
        batch_id = order_ref[t]
        table_high, table_low = split(jnp.concatenate([root_ref[batch_id], gain_ref[batch_id]], axis=0))
        both = nn(table_high, jnp.concatenate([high, low], axis=1))
        part = both[:, :LANES] + both[:, LANES:] + nn(table_low, high)
        lane = lane_ids((quarter, LANES))
        weighted = jnp.where(lane < members, part[:quarter], jnp.where(lane == members, -part[quarter:], 0.0))
        mine = pl.ds(pl.multiple_of(band * quarter, quarter), quarter)
        v_s[t, mine, :] = weighted * (1.0 / (members - 1.0))

        def copy(k):
            return pltpu.make_async_remote_copy(
                src_ref=v_s.at[t, mine, :],
                dst_ref=v_s.at[t, mine, :],
                send_sem=send_sem.at[t, k - 1],
                recv_sem=recv_sem.at[t, k - 1],
                device_id={"gy": lax.rem(band + k, bands)},
                device_id_type=MESH,
            )

        for k in range(1, bands):
            copy(k).start()

        z3_s[lax.rem(t, 2)] = prior_wide(prior)

        before = jnp.maximum(t - 1, 0)
        past = lax.rem(t + 1, 2)
        rows = obs_s[at(t + 1), :]
        rows = update(rows, obs_taper(rows, before), before, past)
        obs_s[at(t + 1), :] = rows
        gained = nt(state_wide(rows), z3_s[lax.rem(t, 2)]) * obs_taper(rows, t)
        gh_s[...], gl_s[...] = split(gained)
        update_cells(before, past)

        def later(i, _):
            here = pl.ds(pl.multiple_of((t + 2 + 2 * i) * obs, obs), 2 * obs)
            rows = obs_s[here, :]
            obs_s[here, :] = update(rows, obs_taper(rows, before), before, past)
            return 0

        lax.fori_loop(0, (batches - 1 - t) // 2 * jnp.minimum(t, 1), later, 0)

        for k in range(1, bands):
            copy(k).wait()

        vw_s[...] = jnp.concatenate(split(v_s[t]), axis=1)

        obs_s[at(t + 1), :] = apply(obs_s[at(t + 1), :], gh_s[...], gl_s[...])
        return 0

    lax.fori_loop(0, batches, turn, 0)
    update_cells(batches - 1, (batches - 1) % 2)
    for c in range(classes):
        tall = cells_s[pl.ds(c * levels, levels), :].T
        anom_out[:, c, :] = tall[:members]
        mean_out[pl.ds(c, 1), :] = tall[members:members + 1]


def wide_local(anomalies, state_mean, obs_value, obs_cell, owner, order, root_inv, gain_inv):
    members, lon_dev, lat_dev, levels = anomalies.shape
    classes = lon_dev * lat_dev
    cells = classes * levels
    batches, quarter = obs_value.shape
    obs = obs_cell.shape[1]
    slabs, bands = lax.axis_size("gx"), lax.axis_size("gy")
    chunk = batches * quarter // slabs
    height = (members + 4 + 7) // 8 * 8
    state, rows = pl.pallas_call(
        functools.partial(pick_kernel, lon_dev, lat_dev),
        out_shape=(
            jax.ShapeDtypeStruct((cells, LANES), F32),
            jax.ShapeDtypeStruct((slabs, height, chunk), F32),
        ),
        in_specs=[SMEM] * 4 + [VMEM] * 2,
        out_specs=(VMEM, VMEM),
        scratch_shapes=[pltpu.VMEM((batches * quarter, LANES), F32)],
        name="pick",
    )(
        obs_cell, obs_value, owner, order,
        anomalies.reshape(members, classes, levels), state_mean.reshape(classes, levels),
    )

    rows = pl.pallas_call(
        functools.partial(spread_kernel, bands, slabs),
        out_shape=jax.ShapeDtypeStruct((bands, slabs, height, chunk), F32),
        in_specs=[VMEM],
        out_specs=VMEM,
        scratch_shapes=[pltpu.VMEM((slabs, height, chunk), F32)] + [pltpu.SemaphoreType.DMA((slabs,))] * 10,
        compiler_params=pltpu.CompilerParams(collective_id=1, has_side_effects=True),
        name="spread",
    )(rows)

    sizes = (
        members, lon_dev, lat_dev, levels, float(slabs * lon_dev), float(bands * lat_dev), REACH * lon_dev + 1.0, bands
    )
    post, mean = pl.pallas_call(
        functools.partial(main_kernel, sizes),
        out_shape=(
            jax.ShapeDtypeStruct((members, classes, levels), F32),
            jax.ShapeDtypeStruct((classes, levels), F32),
        ),
        in_specs=[SMEM] * 2 + [VMEM] * 5,
        out_specs=(VMEM, VMEM),
        scratch_shapes=[
            pltpu.VMEM((batches, 1, obs), F32),
            pltpu.VMEM((batches, 1, obs), F32),
            pltpu.VMEM((cells, LANES), F32),
            pltpu.VMEM(((batches + 2) * obs, LANES), F32),
            pltpu.VMEM((batches, obs, LANES), F32),
            pltpu.VMEM((obs, 2 * LANES), BF16),
            pltpu.VMEM((2, obs, 2 * LANES), BF16),
            pltpu.VMEM((obs, obs), BF16),
            pltpu.VMEM((obs, obs), BF16),
            pltpu.SemaphoreType.DMA((batches, bands - 1)),
            pltpu.SemaphoreType.DMA((batches, bands - 1)),
        ],
        compiler_params=pltpu.CompilerParams(collective_id=0, has_side_effects=True),
        name="analysis",
    )(
        order, owner, state, rows, obs_cell, root_inv, gain_inv,
    )
    return post.reshape(members, lon_dev, lat_dev, levels), mean.reshape(lon_dev, lat_dev, levels)


def analysis_kernel(
    sizes, index_ref, order_ref, owner_ref, cell_ref, value_ref, anom_ref, mean_ref, root_ref, gain_ref,
    cells_s,
    lat_ref, lon_ref, pick_s, packed_s, land, mine_s, share_s, obs_s, full_s, th_s, tl_s, z3_s, vw_s,
    rs_send, rs_recv, send1, recv1, send2, recv2, send3, recv3, near_send, near_recv, far_send, far_recv, hand_send, hand_recv,
):
    members, lon_dev, lat_dev, levels, lon_total, lat_total, span, bands, slabs, early = sizes
    batches, obs = cell_ref.shape
    quarter, half = obs // bands, obs // 2
    piece = quarter // slabs
    ahead, prompt = min(6, batches), min(4, batches)
    column, band = lax.axis_index("gx"), lax.axis_index("gy")
    partner = band + 1 - 2 * lax.rem(band, 2)
    across = lax.rem(band + bands // 2, bands)
    near = lax.div(band, bands // 2)
    far = 1 - near
    classes = lon_dev * lat_dev
    chunk = 8

    def slab(k):
        return lax.rem(column + k, slabs)

    def band_rows(b):
        return pl.ds(pl.multiple_of(b * quarter, quarter), quarter)

    def half_rows(h):
        return pl.ds(pl.multiple_of(h * half, half), half)

    def remote(src, dst, send, recv, device):
        return pltpu.make_async_remote_copy(
            src_ref=src, dst_ref=dst, send_sem=send, recv_sem=recv, device_id=device, device_id_type=MESH
        )

    ends = (0, 3, early + 2, batches)

    def part_rows(p):
        return pl.ds(ends[p] * piece, (ends[p + 1] - ends[p]) * piece)

    def reduce_copy(k, p):
        here = part_rows(p)
        return remote(
            packed_s.at[slab(k), here], land.at[k, here], rs_send.at[p, k], rs_recv.at[p, k], {"gx": slab(k)}
        )

    def my_piece(s):
        return pl.ds(pl.multiple_of(s * piece, piece), piece)

    rank, side = lax.div(column, 2), lax.rem(column, 2)
    ranks = slabs // 2

    def keep(s):
        rows = mine_s[my_piece(s), :]
        share_s[s] = rows
        obs_s[s, band, rank, side] = rows

        def start(device):
            remote(share_s.at[s], obs_s.at[s, band, rank, side], send1.at[s], recv1.at[s], device).start()

        return start

    def share_ranks(s):
        start = keep(s)
        for k in range(1, ranks):
            start({"gx": 2 * lax.rem(rank + k, ranks) + side})

    def share_sides(s):
        pieces(s, ranks - 1, recv1)
        place = obs_s.at[s, band, :, side]
        for target in ({"gx": 2 * rank + 1 - side}, {"gy": across}, {"gx": 2 * rank + 1 - side, "gy": across}):
            remote(place, place, send3.at[s], recv3.at[s], target).start()

    def share(s):
        start = keep(s)

        for k in range(1, slabs):
            start({"gx": slab(k)})
        for k in range(slabs):
            start({"gx": slab(k), "gy": across})

    def pieces(s, count, sem):
        window = mine_s.at[pl.ds(0, count * piece)]
        pltpu.make_async_copy(window, window, sem.at[s]).wait()

    def shared(s, sem):
        pieces(s, 2 * slabs - 1, sem)

    def pass_on(s, i):
        place = obs_s.at[s, (band, across)[i]]
        return remote(place, place, send2.at[s, i], recv2.at[s, i], {"gy": partner})

    def near_copy(t):
        return remote(
            full_s.at[t, :, :, band_rows(band)], full_s.at[t, :, :, band_rows(band)], near_send.at[t], near_recv.at[t], {"gy": partner}
        )

    def far_copy(t):
        return remote(
            full_s.at[t, :, near, band_rows(band)], full_s.at[t, :, near, band_rows(band)], far_send.at[t],
            far_recv.at[t], {"gy": across},
        )

    def hand_copy(t):
        place = full_s.at[t, :, far, band_rows(across)]
        return remote(place, place, hand_send.at[t], hand_recv.at[t], {"gy": partner})

    def send_table(t):
        far_copy(t).start()
        near_copy(t).start()

    def hand_table(t):
        far_copy(t).wait_recv()
        hand_copy(t).start()

    def prepare(t, slot):
        for k in range(2):
            aside = full_s[t, k, far, half_rows(near), :]
            blocks = (
                (near, near, full_s[t, k, near, half_rows(near), :]),
                (far, near, aside),
                (near, far, aside.T),
                (far, far, full_s[t, k, far, half_rows(far), :]),
            )
            for columns, rows, block in blocks:
                here = pl.ds(pl.multiple_of(k * obs + rows * half, half), half)
                high, low = split(block)
                th_s[slot, columns, here, :] = high
                tl_s[slot, columns, here, :] = low

    barrier = pltpu.get_barrier_semaphore()
    for k in range(1, slabs):
        pl.semaphore_signal(barrier, inc=1, device_id={"gx": slab(k)}, device_id_type=MESH)
    for k in range(slabs):
        pl.semaphore_signal(barrier, inc=1, device_id={"gx": slab(k), "gy": across}, device_id_type=MESH)
    pl.semaphore_signal(barrier, inc=1, device_id={"gy": partner}, device_id_type=MESH)

    for c in range(classes):
        lat = (band * lat_dev + c % lat_dev).astype(F32) * (1.0 / lat_total)
        lon = (column * lon_dev + c // lat_dev).astype(F32)
        tall = jnp.concatenate(
            [
                anom_ref[:, c, :],
                mean_ref[pl.ds(c, 1), :],
                jnp.full((1, levels), lat, F32),
                jnp.full((1, levels), lon, F32),
                jnp.zeros((1, levels), F32),
                jnp.full((1, levels), float(c // lat_dev), F32),
                jnp.zeros((LANES - members - 5, levels), F32),
            ],
            axis=0,
        )
        cells_s[pl.ds(c * levels, levels), :] = tall.T

    def pick(t, _):
        b = order_ref[t]
        for j in range(quarter):
            pick_s[pl.ds(j, 1), :] = cells_s[pl.ds(index_ref[b, band * quarter + j], 1), :]
        block = pick_s[...]
        values = jnp.broadcast_to(value_ref[pl.ds(b, 1), :], (LANES, quarter)).T
        block = jnp.where(lane_ids(block.shape) == members + 3, values, block)
        block = jnp.where(owner_ref[b] == column, block, 0.0)
        packed_s[:, my_piece(t), :] = block.reshape(slabs, piece, LANES)
        return 0

    def spread_part(p):
        for k in range(1, slabs):
            reduce_copy(k, p).start()

    def stage(t, _):
        b = order_ref[t]
        for h in range(2):
            full_s[t, 0, h, band_rows(band), :] = root_ref[b, :, h * half:(h + 1) * half]
            full_s[t, 1, h, band_rows(band), :] = gain_ref[b, :, h * half:(h + 1) * half]
        return 0

    lax.fori_loop(ends[0], ends[1], pick, 0)
    pl.semaphore_wait(barrier, 2 * slabs)
    spread_part(0)
    stage(0, 0)
    send_table(0)
    lax.fori_loop(ends[1], ends[2], pick, 0)
    spread_part(1)
    lax.fori_loop(1, batches, stage, 0)
    for t in range(1, prompt):
        send_table(t)
    lax.fori_loop(ends[2], ends[3], pick, 0)

    first_lat = lax.broadcasted_iota(jnp.int32, (1, obs), 1).astype(F32)
    first_lat = jnp.floor((first_lat + 0.5) * (1.0 / quarter)) * lat_dev
    for t in range(batches):
        batch_id = order_ref[t]
        level_row = jnp.floor((cell_ref[pl.ds(batch_id, 1), :].astype(F32) + 0.5) * (1.0 / levels))
        lon_row = jnp.floor((level_row + 0.5) * (1.0 / lat_dev))
        lat_ref[t + early] = (level_row - lon_row * lat_dev + first_lat) * (1.0 / lat_total)
        lon_ref[t + early] = lon_row + (owner_ref[batch_id] * lon_dev).astype(F32)
    for t in range(early):
        lat_ref[t] = jnp.zeros((1, obs), F32)
        lon_ref[t] = jnp.zeros((1, obs), F32)
        vw_s[t] = jnp.zeros(vw_s.shape[1:], BF16)
        z3_s[t] = jnp.zeros(z3_s.shape[1:], BF16)
    for s in range(batches, obs_s.shape[0]):
        obs_s[s] = jnp.zeros(obs_s.shape[1:], F32)
    mine_s[...] = jnp.zeros_like(mine_s)

    def collect(p):
        here = part_rows(p)
        total = packed_s[column, here, :]
        for k in range(1, slabs):
            reduce_copy(k, p).wait_recv()
            total = total + land[k, here, :]
        return total

    mine_s[part_rows(0), :] = collect(0)
    for s in range(ends[1]):
        share_ranks(s)
    mine_s[part_rows(1), :] = collect(1)
    for s in range(ends[1], early):
        share(s)
    spread_part(2)
    for s in range(ends[1]):
        share_sides(s)
    for t in range(prompt, ahead):
        send_table(t)
    hand_table(0)
    near_copy(0).wait_recv()
    hand_copy(0).wait_recv()
    prepare(0, 0)

    def pass_both(s):
        for i in range(2):
            pass_on(s, i).start()

    def passed(s):
        for i in range(2):
            pass_on(s, i).wait()

    for s in range(2):
        pieces(s, 3 * ranks, recv3)
        pass_both(s)
    for t in range(1, 3):
        hand_table(t)
    for s in range(2):
        passed(s)
    pieces(2, 3 * ranks, recv3)
    for s in range(ends[1]):
        pieces(s, 3 * ranks, send3)

    def state_wide(value):
        low = value - value.astype(BF16).astype(F32)
        lane = lane_ids(value.shape)
        room = LANES - members
        moved = pltpu.roll(low, members, 1)
        first = jnp.where(lane < members, value, moved)
        last = jnp.where(lane < members - room, moved, pltpu.roll(value, members - room, 1))
        return jnp.concatenate([first.astype(BF16), last.astype(BF16)], axis=1)

    def prior_tall(prior):
        high, low = split(prior.T[:members])
        return jnp.concatenate([high, high, low, jnp.zeros((2 * LANES - 3 * members, obs), BF16)], axis=0)

    def lon_weight(gap):
        gap = jnp.abs(gap)
        gap = jnp.minimum(gap, lon_total - gap)
        return jnp.maximum(0.0, 1.0 - gap * (1.0 / span))

    def lat_weight(gap):
        return 1.0 - jnp.abs(gap)

    def apply(rows, high, low, vw):
        both = nn(jnp.concatenate([high, low], axis=1), vw)
        return rows - (both[:, :LANES] + both[:, LANES:])

    def tall(high, low):
        under = jnp.concatenate([high, jnp.zeros_like(high)], axis=1)
        return jnp.concatenate([jnp.concatenate([high, low], axis=1), under], axis=0)

    def gain_of(rows, taper, z3):
        return split(nn(state_wide(rows), z3) * taper)

    def update(rows, taper, z3, vw):
        high, low = gain_of(rows, taper, z3)
        return apply(rows, high, low, vw)

    def obs_taper(lat, bit, s, e):
        lon = (owner_ref[order_ref[jnp.minimum(s, batches - 1)]] * lon_dev).astype(F32)
        west = lon_weight(lon - lon_ref[e])
        east = lon_weight(lon + 1.0 - lon_ref[e])
        return lat_weight(lat - lat_ref[e]) * (west + bit * (east - west))

    def mine_taper(rows, e):
        lat, lon = rows[:, members + 1:members + 2], rows[:, members + 2:members + 3]
        return lat_weight(lat - lat_ref[e]) * lon_weight(lon - lon_ref[e])

    def update_mine(rows, e, z3, vw):
        return update(rows, mine_taper(rows, e), z3, vw)

    def update_cells(e, part):
        tapers = []
        for k in range(chunk):
            c = part * chunk + k
            lat = (band * lat_dev + c % lat_dev).astype(F32) * (1.0 / lat_total)
            lon = (column * lon_dev + c // lat_dev).astype(F32)
            weight = lat_weight(lat - lat_ref[e]) * lon_weight(lon - lon_ref[e])
            tapers.append(jnp.broadcast_to(weight, (levels, obs)))
        here = pl.ds(part * chunk * levels, chunk * levels)
        cells_s[here, :] = update(cells_s[here, :], jnp.concatenate(tapers, axis=0), z3_s[e], vw_s[e])

    cell_parts = classes // chunk

    def turn(t, _):
        slot = lax.rem(t, 2)
        e = t + early

        @pl.when(t == ends[2] - early)
        def _():
            rows = collect(2)
            for k in range(ends[2] - early):
                rows = update_mine(rows, early + k, z3_s[early + k], vw_s[early + k])
            mine_s[part_rows(2), :] = rows

        @pl.when(e < batches)
        def _():
            share(e)

        @pl.when(t + 2 < batches)
        def _():
            pass_both(t + 2)

        @pl.when(t + 3 < batches)
        def _():
            shared(t + 3, recv1)

        @pl.when(t + ahead < batches)
        def _():
            send_table(t + ahead)

        @pl.when(t + 3 < batches)
        def _():
            hand_table(t + 3)

        @pl.when(t + 1 < batches)
        def _():
            near_copy(t + 1).wait_recv()
            hand_copy(t + 1).wait_recv()

        @pl.when(jnp.logical_and(t > 0, t + 1 < batches))
        def _():
            passed(t + 1)

        prior = obs_s[t].reshape(obs, LANES)
        rows = obs_s[t + 1].reshape(obs, LANES)
        coming = t + 3
        later = jnp.concatenate(
            [obs_s[coming, place].reshape(quarter, LANES) for place in (band, across)], axis=0
        )
        lat, bit = rows[:, members + 1:members + 2], rows[:, members + 4:members + 5]
        later_lat, later_bit = later[:, members + 1:members + 2], later[:, members + 4:members + 5]
        done = 0

        def some_cells(upto):
            nonlocal done
            while done < min(upto, cell_parts):
                update_cells(e - 1, done)
                done += 1

        def catch_up(later, k, z3, vw):
            return update(later, obs_taper(later_lat, later_bit, coming, e - k), z3, vw)

        lane = lane_ids(prior.shape)
        innovation = pltpu.roll(prior, LANES - 3, 1) - prior
        joined = jnp.where(lane < members, prior, jnp.where(lane == members, innovation, 0.0))
        high, low = split(joined)
        table_high = jnp.concatenate([th_s[slot, 0], th_s[slot, 1]], axis=1)
        table_low = jnp.concatenate([tl_s[slot, 0], tl_s[slot, 1]], axis=1)
        both = nn(jnp.concatenate([table_high, table_low], axis=1), tall(high, low))
        part = both[:, :LANES] + both[:, LANES:]
        lane = lane_ids((obs, LANES))
        weighted = jnp.where(lane < members, part[:obs], jnp.where(lane == members, -part[obs:], 0.0))
        vw = tall(*split(weighted * (1.0 / (members - 1.0))))
        z3 = prior_tall(prior)

        later = catch_up(later, 2, z3_s[e - 2], vw_s[e - 2])
        tapers = (obs_taper(lat, bit, t + 1, e - 1), obs_taper(later_lat, later_bit, coming, e - 1))
        both = update(jnp.concatenate([rows, later], axis=0), jnp.concatenate(tapers, axis=0), z3_s[e - 1], vw_s[e - 1])
        rows, later = both[:obs], both[obs:]
        some_cells(cell_parts)
        mine = mine_s[...]
        joint = jnp.concatenate([rows, later, mine], axis=0)
        tapers = (obs_taper(lat, bit, t + 1, e), obs_taper(later_lat, later_bit, coming, e), mine_taper(mine, e))
        joint = update(joint, jnp.concatenate(tapers, axis=0), z3, vw)
        obs_s[t + 1] = joint[:obs].reshape(obs_s.shape[1:])
        for i, place in enumerate((band, across)):
            obs_s[coming, place] = joint[obs + i * quarter:obs + (i + 1) * quarter].reshape(obs_s.shape[2:])
        mine_s[...] = joint[obs + 2 * quarter:]
        z3_s[e] = z3
        vw_s[e] = vw
        prepare(jnp.minimum(t + 1, batches - 1), 1 - slot)
        return 0

    lax.fori_loop(0, batches, turn, 0)
    for i in range(cell_parts):
        update_cells(batches - 1 + early, i)

    for p in range(3):
        for k in range(1, slabs):
            reduce_copy(k, p).wait_send()

    def sent(t, _):
        near_copy(t).wait_send()
        far_copy(t).wait_send()
        hand_copy(t).wait_send()
        return 0

    lax.fori_loop(0, batches, sent, 0)
    for s in range(ends[1]):
        pieces(s, ranks - 1, send1)

    def shared_sent(s, _):
        shared(s, send1)
        return 0

    lax.fori_loop(ends[1], batches, shared_sent, 0)


def finish_kernel(cells_ref, anom_out, mean_out):
    members, classes, levels = anom_out.shape
    for c in range(classes):
        tall = cells_ref[pl.ds(c * levels, levels), :].T
        anom_out[:, c, :] = tall[:members]
        mean_out[pl.ds(c, 1), :] = tall[members:members + 1]


def near_local(anomalies, state_mean, obs_value, obs_cell, owner, order, root_inv, gain_inv):
    members, lon_dev, lat_dev, levels = anomalies.shape
    classes = lon_dev * lat_dev
    cells = classes * levels
    batches, quarter = obs_value.shape
    obs = obs_cell.shape[1]
    half = obs // 2
    slabs, bands = lax.axis_size("gx"), lax.axis_size("gy")
    piece = quarter // slabs
    early = min(EARLY, batches)
    lat_total = float(bands * lat_dev)
    sizes = (
        members, lon_dev, lat_dev, levels, float(slabs * lon_dev), lat_total, REACH * lon_dev + 1.0, bands, slabs, early
    )
    dma = pltpu.SemaphoreType.DMA
    cells_out = pl.pallas_call(
        functools.partial(analysis_kernel, sizes),
        out_shape=jax.ShapeDtypeStruct((cells, LANES), F32),
        in_specs=[SMEM] * 3 + [VMEM] * 6,
        out_specs=VMEM,
        scratch_shapes=[
            pltpu.VMEM((batches + early, 1, obs), F32),
            pltpu.VMEM((batches + early, 1, obs), F32),
            pltpu.VMEM((quarter, LANES), F32),
            pltpu.VMEM((slabs, batches * piece, LANES), F32),
            pltpu.VMEM((slabs, batches * piece, LANES), F32),
            pltpu.VMEM((batches * piece, LANES), F32),
            pltpu.VMEM((batches, piece, LANES), F32),
            pltpu.VMEM((batches + 3, bands, slabs // 2, 2, piece, LANES), F32),
            pltpu.VMEM((batches, 2, 2, obs, half), F32),
            pltpu.VMEM((2, 2, 2 * obs, half), BF16),
            pltpu.VMEM((2, 2, 2 * obs, half), BF16),
            pltpu.VMEM((batches + early, 2 * LANES, obs), BF16),
            pltpu.VMEM((batches + early, 2 * obs, 2 * LANES), BF16),
            dma((3, slabs)), dma((3, slabs)),
            dma((batches,)), dma((batches,)),
            dma((batches, 2)), dma((batches, 2)),
            dma((3,)), dma((3,)),
            dma((batches,)), dma((batches,)),
            dma((batches,)), dma((batches,)),
            dma((batches,)), dma((batches,)),
        ],
        compiler_params=pltpu.CompilerParams(collective_id=0, has_side_effects=True),
        name="analysis",
    )(
        obs_cell, order, owner, obs_cell, obs_value,
        anomalies.reshape(members, classes, levels), state_mean.reshape(classes, levels), root_inv, gain_inv,
    )

    post, mean = pl.pallas_call(
        finish_kernel,
        out_shape=(
            jax.ShapeDtypeStruct((members, classes, levels), F32),
            jax.ShapeDtypeStruct((classes, levels), F32),
        ),
        in_specs=[VMEM],
        out_specs=(VMEM, VMEM),
        name="finish",
    )(cells_out)
    return post.reshape(members, lon_dev, lat_dev, levels), mean.reshape(lon_dev, lat_dev, levels)


def local(*arrays):
    obs_value, obs_cell = arrays[2], arrays[3]
    slabs, bands = lax.axis_size("gx"), lax.axis_size("gy")
    piece = obs_value.shape[1] // slabs
    fits = bands == 4 and piece % 8 == 0 and piece * slabs == obs_value.shape[1] and obs_cell.shape[1] == 2 * LANES
    return (near_local if fits and arrays[0].shape[1] == 2 else wide_local)(*arrays)


def solution(mesh):
    return jax.shard_map(
        local,
        mesh=mesh,
        in_specs=(
            P(None, "gx", "gy", None),
            P("gx", "gy", None),
            P(None, "gy"),
            P(),
            P(),
            P(),
            P(None, "gy", None),
            P(None, "gy", None),
        ),
        out_specs=(P(None, "gx", "gy", None), P("gx", "gy", None)),
        check_vma=False,
    )
```

```python
import functools

import jax
import jax.numpy as jnp
from jax import lax
from jax.experimental import pallas as pl
from jax.experimental.pallas import tpu as pltpu
from jax.sharding import PartitionSpec as P

REACH = 3
EARLY = 5
LANES = 128
MESH = pl.DeviceIdType.MESH
VMEM = pl.BlockSpec(memory_space=pltpu.VMEM)
SMEM = pl.BlockSpec(memory_space=pltpu.SMEM)
F32 = jnp.float32
BF16 = jnp.bfloat16


def split(value):
    high = value.astype(BF16)
    return high, (value - high.astype(F32)).astype(BF16)


def nn(left, right):
    return lax.dot_general(left, right, (((1,), (0,)), ((), ())), preferred_element_type=F32)


def nt(left, right):
    return lax.dot_general(left, right, (((1,), (1,)), ((), ())), preferred_element_type=F32)


def lane_ids(shape):
    return lax.broadcasted_iota(jnp.int32, shape, len(shape) - 1)


def pick_kernel(lon_dev, lat_dev, cells_ref, value_ref, owner_ref, order_ref, anom_ref, mean_ref, state_ref, packed_ref, rows_ref):
    column, band = lax.axis_index("gx"), lax.axis_index("gy")
    members, classes, levels = anom_ref.shape
    batches, quarter = value_ref.shape

    for c in range(classes):
        lat = (band * lat_dev + c % lat_dev).astype(F32)
        lon = (column * lon_dev + c // lat_dev).astype(F32)
        tall = jnp.concatenate(
            [
                anom_ref[:, c, :],
                mean_ref[pl.ds(c, 1), :],
                jnp.full((1, levels), lat, F32),
                jnp.full((1, levels), lon, F32),
                jnp.zeros((LANES - members - 3, levels), F32),
            ],
            axis=0,
        )
        state_ref[pl.ds(c * levels, levels), :] = tall.T

    lane = lane_ids((1, LANES))

    def batch(t, _):
        b = order_ref[t]
        mine = owner_ref[b] == column

        @pl.when(mine)
        def _():
            def group(i, _):
                for k in range(8):
                    j = i * 8 + k
                    row = state_ref[pl.ds(cells_ref[b, band * quarter + j], 1), :]
                    rows_ref[pl.ds(t * quarter + j, 1), :] = jnp.where(lane == members + 3, value_ref[b, j], row)
                return 0

            lax.fori_loop(0, quarter // 8, group, 0)

        @pl.when(jnp.logical_not(mine))
        def _():
            rows_ref[pl.ds(pl.multiple_of(t * quarter, quarter), quarter), :] = jnp.zeros((quarter, LANES), F32)

        return 0

    lax.fori_loop(0, batches, batch, 0)
    slabs, height, chunk = packed_ref.shape
    for q in range(slabs):
        packed_ref[q] = rows_ref[pl.ds(q * chunk, chunk), :].T[:height]


def spread_kernel(bands, slabs, rows_ref, out_ref, land, send1, recv1, send2, recv2, send3, recv3, send4, recv4, send5, recv5):
    x, b = lax.axis_index("gx"), lax.axis_index("gy")
    partner = b + 1 - 2 * lax.rem(b, 2)
    across = lax.rem(b + 2, bands)

    def slab(k):
        return lax.rem(x + k, slabs)

    def source(k):
        return lax.rem(x + slabs - k, slabs)

    def first(k):
        return pltpu.make_async_remote_copy(
            src_ref=rows_ref.at[slab(k)], dst_ref=land.at[k], send_sem=send1.at[k], recv_sem=recv1.at[k],
            device_id={"gx": slab(k)}, device_id_type=MESH,
        )

    def second(k):
        return pltpu.make_async_remote_copy(
            src_ref=out_ref.at[b, x], dst_ref=out_ref.at[b, x], send_sem=send2.at[k],
            recv_sem=recv2.at[k], device_id={"gx": slab(k)}, device_id_type=MESH,
        )

    def hand(k, of_band, send_sem, recv_sem, target):
        place = out_ref.at[of_band, source(k)]
        return pltpu.make_async_remote_copy(
            src_ref=place, dst_ref=place, send_sem=send_sem.at[k], recv_sem=recv_sem.at[k],
            device_id={"gy": target}, device_id_type=MESH,
        )

    def third(k):
        return hand(k, b, send3, recv3, partner)

    def fourth(k):
        return hand(k, b, send4, recv4, across)

    def fifth(k):
        return hand(k, across, send5, recv5, partner)

    def each(low, high, body):
        def step(k, _):
            body(k)
            return 0

        lax.fori_loop(low, high, step, 0)

    barrier = pltpu.get_barrier_semaphore()
    each(1, slabs, lambda k: pl.semaphore_signal(barrier, inc=1, device_id={"gx": slab(k)}, device_id_type=MESH))
    for target in (partner, across):
        pl.semaphore_signal(barrier, inc=1, device_id={"gy": target}, device_id_type=MESH)
    pl.semaphore_wait(barrier, slabs + 1)

    each(1, slabs, lambda k: first(k).start())
    out_ref[b, x] = rows_ref[x]

    def add(k):
        first(k).wait_recv()
        out_ref[b, x] += land[k]

    each(1, slabs, add)
    fourth(0).start()
    each(1, slabs, lambda k: second(k).start())
    third(0).start()

    def relay(k):
        second(k).wait_recv()
        fourth(k).start()
        third(k).start()
        fourth(k - 1).wait_recv()
        fifth(k - 1).start()

    each(1, slabs, relay)
    fourth(slabs - 1).wait_recv()
    fifth(slabs - 1).start()

    def finish(k):
        third(k).wait()
        fifth(k).wait()
        fourth(k).wait_send()

    each(0, slabs, finish)

    def sent(k):
        first(k).wait_send()
        second(k).wait_send()

    each(1, slabs, sent)


def main_kernel(
    sizes, order_ref, owner_ref, state_ref, obs_ref, cell_ref, root_ref, gain_ref,
    anom_out, mean_out,
    lat_ref, lon_ref, cells_s, obs_s, v_s, vw_s, z3_s, gh_s, gl_s, send_sem, recv_sem,
):
    members, lon_dev, lat_dev, levels, lon_total, lat_total, span, bands = sizes
    batches, obs = cell_ref.shape
    quarter = obs // bands
    column, band = lax.axis_index("gx"), lax.axis_index("gy")
    classes = lon_dev * lat_dev
    chunk = 4

    barrier = pltpu.get_barrier_semaphore()
    for k in range(1, bands):
        pl.semaphore_signal(barrier, inc=1, device_id={"gy": lax.rem(band + k, bands)}, device_id_type=MESH)
    pl.semaphore_wait(barrier, bands - 1)

    def widen(value, with_low_in_middle):
        high, low = split(value)
        high, low = high.astype(F32), low.astype(F32)
        second, third = (low, high) if with_low_in_middle else (high, low)
        lane = lane_ids(value.shape)
        room = LANES - members
        moved = pltpu.roll(second, members, 1)
        first = jnp.where(lane < members, high, moved)
        last = jnp.where(lane < members - room, moved, pltpu.roll(third, members - room, 1))
        return jnp.concatenate([first, last], axis=1), lane, room

    def state_wide(value):
        return widen(value, True)[0].astype(BF16)

    def prior_wide(value):
        wide, lane, room = widen(jnp.where(lane_ids(value.shape) < members, value, 0.0), False)
        wide_lane = lane_ids(wide.shape)
        return jnp.where(wide_lane < 3 * members, wide, 0.0).astype(BF16)

    def lon_weight(gap):
        gap = jnp.abs(gap)
        gap = jnp.minimum(gap, lon_total - gap)
        return jnp.maximum(0.0, 1.0 - gap * (1.0 / span))

    def lat_weight(gap):
        return 1.0 - jnp.abs(gap) * (1.0 / lat_total)

    def obs_taper(rows, s):
        lat, lon = rows[:, members + 1:members + 2], rows[:, members + 2:members + 3]
        return lat_weight(lat - lat_ref[s]) * lon_weight(lon - lon_ref[s])

    def apply(rows, high, low):
        both = nn(high, vw_s[...])
        return rows - (both[:, :LANES] + both[:, LANES:] + nn(low, vw_s[:, :LANES]))

    def update(rows, taper, s, slot):
        gained = nt(state_wide(rows), z3_s[slot]) * taper
        return apply(rows, *split(gained))

    def update_cells(s, slot):
        for i in range(classes // chunk):
            tapers = []
            for k in range(chunk):
                c = i * chunk + k
                lat = (band * lat_dev + c % lat_dev).astype(F32)
                lon = (column * lon_dev + c // lat_dev).astype(F32)
                weight = lat_weight(lat - lat_ref[s]) * lon_weight(lon - lon_ref[s])
                tapers.append(jnp.broadcast_to(weight, (levels, obs)))
            here = pl.ds(i * chunk * levels, chunk * levels)
            cells_s[here, :] = update(cells_s[here, :], jnp.concatenate(tapers, axis=0), s, slot)

    def at(t):
        return pl.ds(pl.multiple_of(t * obs, obs), obs)

    cells_s[...] = state_ref[...]
    _, slabs, height, width = obs_ref.shape
    part = min(width, quarter)
    for q in range(bands):
        for p in range(slabs):
            rest = jnp.zeros((LANES - height, width), F32)
            block = jnp.concatenate([obs_ref[q, p], rest], axis=0).T
            for i in range(0, width, part):
                t, j = divmod(p * width + i, quarter)
                obs_s[pl.ds(t * obs + q * quarter + j, part), :] = block[i:i + part]
    obs_s[pl.ds(batches * obs, 2 * obs), :] = jnp.zeros((2 * obs, LANES), F32)
    vw_s[...] = jnp.zeros_like(vw_s)
    z3_s[...] = jnp.zeros_like(z3_s)
    first_lat = lax.broadcasted_iota(jnp.int32, (1, obs), 1).astype(F32)
    first_lat = jnp.floor((first_lat + 0.5) * (1.0 / quarter)) * lat_dev
    for t in range(batches):
        batch_id = order_ref[t]
        level_row = jnp.floor((cell_ref[pl.ds(batch_id, 1), :].astype(F32) + 0.5) * (1.0 / levels))
        lon_row = jnp.floor((level_row + 0.5) * (1.0 / lat_dev))
        lat_ref[t] = level_row - lon_row * lat_dev + first_lat
        lon_ref[t] = lon_row + (owner_ref[batch_id] * lon_dev).astype(F32)

    def turn(t, _):
        prior = obs_s[at(t), :]
        lane = lane_ids(prior.shape)
        innovation = pltpu.roll(prior, LANES - 3, 1) - prior
        joined = jnp.where(lane < members, prior, jnp.where(lane == members, innovation, 0.0))
        high, low = split(joined)
        batch_id = order_ref[t]
        table_high, table_low = split(jnp.concatenate([root_ref[batch_id], gain_ref[batch_id]], axis=0))
        both = nn(table_high, jnp.concatenate([high, low], axis=1))
        part = both[:, :LANES] + both[:, LANES:] + nn(table_low, high)
        lane = lane_ids((quarter, LANES))
        weighted = jnp.where(lane < members, part[:quarter], jnp.where(lane == members, -part[quarter:], 0.0))
        mine = pl.ds(pl.multiple_of(band * quarter, quarter), quarter)
        v_s[t, mine, :] = weighted * (1.0 / (members - 1.0))

        def copy(k):
            return pltpu.make_async_remote_copy(
                src_ref=v_s.at[t, mine, :],
                dst_ref=v_s.at[t, mine, :],
                send_sem=send_sem.at[t, k - 1],
                recv_sem=recv_sem.at[t, k - 1],
                device_id={"gy": lax.rem(band + k, bands)},
                device_id_type=MESH,
            )

        for k in range(1, bands):
            copy(k).start()

        z3_s[lax.rem(t, 2)] = prior_wide(prior)

        before = jnp.maximum(t - 1, 0)
        past = lax.rem(t + 1, 2)
        rows = obs_s[at(t + 1), :]
        rows = update(rows, obs_taper(rows, before), before, past)
        obs_s[at(t + 1), :] = rows
        gained = nt(state_wide(rows), z3_s[lax.rem(t, 2)]) * obs_taper(rows, t)
        gh_s[...], gl_s[...] = split(gained)
        update_cells(before, past)

        def later(i, _):
            here = pl.ds(pl.multiple_of((t + 2 + 2 * i) * obs, obs), 2 * obs)
            rows = obs_s[here, :]
            obs_s[here, :] = update(rows, obs_taper(rows, before), before, past)
            return 0

        lax.fori_loop(0, (batches - 1 - t) // 2 * jnp.minimum(t, 1), later, 0)

        for k in range(1, bands):
            copy(k).wait()

        vw_s[...] = jnp.concatenate(split(v_s[t]), axis=1)

        obs_s[at(t + 1), :] = apply(obs_s[at(t + 1), :], gh_s[...], gl_s[...])
        return 0

    lax.fori_loop(0, batches, turn, 0)
    update_cells(batches - 1, (batches - 1) % 2)
    for c in range(classes):
        tall = cells_s[pl.ds(c * levels, levels), :].T
        anom_out[:, c, :] = tall[:members]
        mean_out[pl.ds(c, 1), :] = tall[members:members + 1]


def wide_local(anomalies, state_mean, obs_value, obs_cell, owner, order, root_inv, gain_inv):
    members, lon_dev, lat_dev, levels = anomalies.shape
    classes = lon_dev * lat_dev
    cells = classes * levels
    batches, quarter = obs_value.shape
    obs = obs_cell.shape[1]
    slabs, bands = lax.axis_size("gx"), lax.axis_size("gy")
    chunk = batches * quarter // slabs
    height = (members + 4 + 7) // 8 * 8
    state, rows = pl.pallas_call(
        functools.partial(pick_kernel, lon_dev, lat_dev),
        out_shape=(
            jax.ShapeDtypeStruct((cells, LANES), F32),
            jax.ShapeDtypeStruct((slabs, height, chunk), F32),
        ),
        in_specs=[SMEM] * 4 + [VMEM] * 2,
        out_specs=(VMEM, VMEM),
        scratch_shapes=[pltpu.VMEM((batches * quarter, LANES), F32)],
        name="pick",
    )(
        obs_cell, obs_value, owner, order,
        anomalies.reshape(members, classes, levels), state_mean.reshape(classes, levels),
    )

    rows = pl.pallas_call(
        functools.partial(spread_kernel, bands, slabs),
        out_shape=jax.ShapeDtypeStruct((bands, slabs, height, chunk), F32),
        in_specs=[VMEM],
        out_specs=VMEM,
        scratch_shapes=[pltpu.VMEM((slabs, height, chunk), F32)] + [pltpu.SemaphoreType.DMA((slabs,))] * 10,
        compiler_params=pltpu.CompilerParams(collective_id=1, has_side_effects=True),
        name="spread",
    )(rows)

    sizes = (
        members, lon_dev, lat_dev, levels, float(slabs * lon_dev), float(bands * lat_dev), REACH * lon_dev + 1.0, bands
    )
    post, mean = pl.pallas_call(
        functools.partial(main_kernel, sizes),
        out_shape=(
            jax.ShapeDtypeStruct((members, classes, levels), F32),
            jax.ShapeDtypeStruct((classes, levels), F32),
        ),
        in_specs=[SMEM] * 2 + [VMEM] * 5,
        out_specs=(VMEM, VMEM),
        scratch_shapes=[
            pltpu.VMEM((batches, 1, obs), F32),
            pltpu.VMEM((batches, 1, obs), F32),
            pltpu.VMEM((cells, LANES), F32),
            pltpu.VMEM(((batches + 2) * obs, LANES), F32),
            pltpu.VMEM((batches, obs, LANES), F32),
            pltpu.VMEM((obs, 2 * LANES), BF16),
            pltpu.VMEM((2, obs, 2 * LANES), BF16),
            pltpu.VMEM((obs, obs), BF16),
            pltpu.VMEM((obs, obs), BF16),
            pltpu.SemaphoreType.DMA((batches, bands - 1)),
            pltpu.SemaphoreType.DMA((batches, bands - 1)),
        ],
        compiler_params=pltpu.CompilerParams(collective_id=0, has_side_effects=True),
        name="analysis",
    )(
        order, owner, state, rows, obs_cell, root_inv, gain_inv,
    )
    return post.reshape(members, lon_dev, lat_dev, levels), mean.reshape(lon_dev, lat_dev, levels)


def analysis_kernel(
    sizes, index_ref, order_ref, owner_ref, cell_ref, value_ref, anom_ref, mean_ref, root_ref, gain_ref,
    cells_s,
    lat_ref, lon_ref, pick_s, packed_s, land, mine_s, share_s, obs_s, full_s, th_s, tl_s, z3_s, vw_s,
    rs_send, rs_recv, send1, recv1, send2, recv2, send3, recv3, near_send, near_recv, far_send, far_recv, hand_send, hand_recv,
):
    members, lon_dev, lat_dev, levels, lon_total, lat_total, span, bands, slabs, early = sizes
    batches, obs = cell_ref.shape
    quarter, half = obs // bands, obs // 2
    piece = quarter // slabs
    ahead, prompt = min(8, batches), min(6, batches)
    column, band = lax.axis_index("gx"), lax.axis_index("gy")
    partner = band + 1 - 2 * lax.rem(band, 2)
    across = lax.rem(band + bands // 2, bands)
    near = lax.div(band, bands // 2)
    far = 1 - near
    classes = lon_dev * lat_dev
    chunk = 8

    def slab(k):
        return lax.rem(column + k, slabs)

    def band_rows(b):
        return pl.ds(pl.multiple_of(b * quarter, quarter), quarter)

    def half_rows(h):
        return pl.ds(pl.multiple_of(h * half, half), half)

    def remote(src, dst, send, recv, device):
        return pltpu.make_async_remote_copy(
            src_ref=src, dst_ref=dst, send_sem=send, recv_sem=recv, device_id=device, device_id_type=MESH
        )

    ends = (0, 3, early + 2, batches)

    def part_rows(p):
        return pl.ds(ends[p] * piece, (ends[p + 1] - ends[p]) * piece)

    def reduce_copy(k, p):
        here = part_rows(p)
        return remote(
            packed_s.at[slab(k), here], land.at[k, here], rs_send.at[p, k], rs_recv.at[p, k], {"gx": slab(k)}
        )

    def my_piece(s):
        return pl.ds(pl.multiple_of(s * piece, piece), piece)

    rank, side = lax.div(column, 2), lax.rem(column, 2)
    ranks = slabs // 2

    def keep(s):
        rows = mine_s[my_piece(s), :]
        share_s[s] = rows
        obs_s[s, band, rank, side] = rows

        def start(device):
            remote(share_s.at[s], obs_s.at[s, band, rank, side], send1.at[s], recv1.at[s], device).start()

        return start

    def share_ranks(s):
        start = keep(s)
        for k in range(1, ranks):
            start({"gx": 2 * lax.rem(rank + k, ranks) + side})

    def share_sides(s):
        pieces(s, ranks - 1, recv1)
        place = obs_s.at[s, band, :, side]
        for target in ({"gx": 2 * rank + 1 - side}, {"gy": across}, {"gx": 2 * rank + 1 - side, "gy": across}):
            remote(place, place, send3.at[s], recv3.at[s], target).start()

    def share(s):
        start = keep(s)
        for k in range(slabs // 2, slabs + slabs // 2):
            start({"gx": slab(k % slabs), "gy": across})
        for k in range(1, slabs):
            start({"gx": slab((k + slabs // 2 - 1) % (slabs - 1) + 1)})

    def pieces(s, count, sem):
        window = mine_s.at[pl.ds(0, count * piece)]
        pltpu.make_async_copy(window, window, sem.at[s]).wait()

    def shared(s, sem):
        pieces(s, 2 * slabs - 1, sem)

    def pass_on(s, i):
        place = obs_s.at[s, (band, across)[i]]
        return remote(place, place, send2.at[s, i], recv2.at[s, i], {"gy": partner})

    def near_copy(t):
        return remote(
            full_s.at[t, :, :, band_rows(band)], full_s.at[t, :, :, band_rows(band)], near_send.at[t], near_recv.at[t], {"gy": partner}
        )

    def far_copy(t):
        return remote(
            full_s.at[t, :, near, band_rows(band)], full_s.at[t, :, near, band_rows(band)], far_send.at[t],
            far_recv.at[t], {"gy": across},
        )

    def hand_copy(t):
        place = full_s.at[t, :, far, band_rows(across)]
        return remote(place, place, hand_send.at[t], hand_recv.at[t], {"gy": partner})

    def send_table(t):
        far_copy(t).start()
        near_copy(t).start()

    def hand_table(t):
        far_copy(t).wait_recv()
        hand_copy(t).start()

    def prepare(t, slot):
        for k in range(2):
            aside = full_s[t, k, far, half_rows(near), :]
            blocks = (
                (near, near, full_s[t, k, near, half_rows(near), :]),
                (far, near, aside),
                (near, far, aside.T),
                (far, far, full_s[t, k, far, half_rows(far), :]),
            )
            for columns, rows, block in blocks:
                here = pl.ds(pl.multiple_of(k * obs + rows * half, half), half)
                high, low = split(block)
                th_s[slot, columns, here, :] = high
                tl_s[slot, columns, here, :] = low

    barrier = pltpu.get_barrier_semaphore()
    for k in range(1, slabs):
        pl.semaphore_signal(barrier, inc=1, device_id={"gx": slab(k)}, device_id_type=MESH)
    for k in range(slabs):
        pl.semaphore_signal(barrier, inc=1, device_id={"gx": slab(k), "gy": across}, device_id_type=MESH)
    pl.semaphore_signal(barrier, inc=1, device_id={"gy": partner}, device_id_type=MESH)

    for c in range(classes):
        lat = (band * lat_dev + c % lat_dev).astype(F32) * (1.0 / lat_total)
        lon = (column * lon_dev + c // lat_dev).astype(F32)
        tall = jnp.concatenate(
            [
                anom_ref[:, c, :],
                mean_ref[pl.ds(c, 1), :],
                jnp.full((1, levels), lat, F32),
                jnp.full((1, levels), lon, F32),
                jnp.zeros((1, levels), F32),
                jnp.full((1, levels), float(c // lat_dev), F32),
                jnp.zeros((LANES - members - 5, levels), F32),
            ],
            axis=0,
        )
        cells_s[pl.ds(c * levels, levels), :] = tall.T

    def pick(t, _):
        b = order_ref[t]
        for j in range(quarter):
            pick_s[pl.ds(j, 1), :] = cells_s[pl.ds(index_ref[b, band * quarter + j], 1), :]
        block = pick_s[...]
        values = jnp.broadcast_to(value_ref[pl.ds(b, 1), :], (LANES, quarter)).T
        block = jnp.where(lane_ids(block.shape) == members + 3, values, block)
        block = jnp.where(owner_ref[b] == column, block, 0.0)
        packed_s[:, my_piece(t), :] = block.reshape(slabs, piece, LANES)
        return 0

    def spread_part(p):
        for k in range(1, slabs):
            reduce_copy(k, p).start()

    def stage(t, _):
        b = order_ref[t]
        for h in range(2):
            full_s[t, 0, h, band_rows(band), :] = root_ref[b, :, h * half:(h + 1) * half]
            full_s[t, 1, h, band_rows(band), :] = gain_ref[b, :, h * half:(h + 1) * half]
        return 0

    lax.fori_loop(ends[0], ends[1], pick, 0)
    pl.semaphore_wait(barrier, 2 * slabs)
    spread_part(0)
    stage(0, 0)
    send_table(0)
    lax.fori_loop(ends[1], ends[2], pick, 0)
    spread_part(1)
    lax.fori_loop(1, batches, stage, 0)
    for t in range(1, prompt):
        send_table(t)
    lax.fori_loop(ends[2], ends[3], pick, 0)

    first_lat = lax.broadcasted_iota(jnp.int32, (1, obs), 1).astype(F32)
    first_lat = jnp.floor((first_lat + 0.5) * (1.0 / quarter)) * lat_dev
    for t in range(batches):
        batch_id = order_ref[t]
        level_row = jnp.floor((cell_ref[pl.ds(batch_id, 1), :].astype(F32) + 0.5) * (1.0 / levels))
        lon_row = jnp.floor((level_row + 0.5) * (1.0 / lat_dev))
        lat_ref[t + early] = (level_row - lon_row * lat_dev + first_lat) * (1.0 / lat_total)
        lon_ref[t + early] = lon_row + (owner_ref[batch_id] * lon_dev).astype(F32)
    for t in range(early):
        lat_ref[t] = jnp.zeros((1, obs), F32)
        lon_ref[t] = jnp.zeros((1, obs), F32)
        vw_s[t] = jnp.zeros(vw_s.shape[1:], BF16)
        z3_s[t] = jnp.zeros(z3_s.shape[1:], BF16)
    for s in range(batches, obs_s.shape[0]):
        obs_s[s] = jnp.zeros(obs_s.shape[1:], F32)
    mine_s[...] = jnp.zeros_like(mine_s)

    def collect(p):
        here = part_rows(p)
        total = packed_s[column, here, :]
        for k in range(1, slabs):
            reduce_copy(k, p).wait_recv()
            total = total + land[k, here, :]
        return total

    mine_s[part_rows(0), :] = collect(0)
    for s in range(ends[1]):
        share_ranks(s)
    mine_s[part_rows(1), :] = collect(1)
    for s in range(ends[1], early):
        share(s)
    spread_part(2)
    for s in range(ends[1]):
        share_sides(s)
    for t in range(prompt, ahead):
        send_table(t)
    hand_table(0)
    near_copy(0).wait_recv()
    hand_copy(0).wait_recv()
    prepare(0, 0)

    def pass_both(s):
        for i in range(2):
            pass_on(s, i).start()

    def passed(s):
        for i in range(2):
            pass_on(s, i).wait()

    for s in range(2):
        pieces(s, 3 * ranks, recv3)
        pass_both(s)
    for t in range(1, 3):
        hand_table(t)
    for s in range(2):
        passed(s)
    pieces(2, 3 * ranks, recv3)
    for s in range(ends[1]):
        pieces(s, 3 * ranks, send3)

    def state_wide(value):
        low = value - value.astype(BF16).astype(F32)
        lane = lane_ids(value.shape)
        room = LANES - members
        moved = pltpu.roll(low, members, 1)
        first = jnp.where(lane < members, value, moved)
        last = jnp.where(lane < members - room, moved, pltpu.roll(value, members - room, 1))
        return jnp.concatenate([first.astype(BF16), last.astype(BF16)], axis=1)

    def prior_tall(prior):
        high, low = split(prior.T[:members])
        return jnp.concatenate([high, high, low, jnp.zeros((2 * LANES - 3 * members, obs), BF16)], axis=0)

    def lon_weight(gap):
        gap = jnp.abs(gap)
        gap = jnp.minimum(gap, lon_total - gap)
        return jnp.maximum(0.0, 1.0 - gap * (1.0 / span))

    def lat_weight(gap):
        return 1.0 - jnp.abs(gap)

    def apply(rows, high, low, vw):
        both = nn(jnp.concatenate([high, low], axis=1), vw)
        return rows - (both[:, :LANES] + both[:, LANES:])

    def tall(high, low):
        under = jnp.concatenate([high, jnp.zeros_like(high)], axis=1)
        return jnp.concatenate([jnp.concatenate([high, low], axis=1), under], axis=0)

    def gain_of(rows, taper, z3):
        return split(nn(state_wide(rows), z3) * taper)

    def update(rows, taper, z3, vw):
        high, low = gain_of(rows, taper, z3)
        return apply(rows, high, low, vw)

    def obs_taper(lat, bit, s, e):
        lon = (owner_ref[order_ref[jnp.minimum(s, batches - 1)]] * lon_dev).astype(F32)
        west = lon_weight(lon - lon_ref[e])
        east = lon_weight(lon + 1.0 - lon_ref[e])
        return lat_weight(lat - lat_ref[e]) * (west + bit * (east - west))

    def mine_taper(rows, e):
        lat, lon = rows[:, members + 1:members + 2], rows[:, members + 2:members + 3]
        return lat_weight(lat - lat_ref[e]) * lon_weight(lon - lon_ref[e])

    def update_mine(rows, e, z3, vw):
        return update(rows, mine_taper(rows, e), z3, vw)

    def update_cells(e, part):
        tapers = []
        for k in range(chunk):
            c = part * chunk + k
            lat = (band * lat_dev + c % lat_dev).astype(F32) * (1.0 / lat_total)
            lon = (column * lon_dev + c // lat_dev).astype(F32)
            weight = lat_weight(lat - lat_ref[e]) * lon_weight(lon - lon_ref[e])
            tapers.append(jnp.broadcast_to(weight, (levels, obs)))
        here = pl.ds(part * chunk * levels, chunk * levels)
        cells_s[here, :] = update(cells_s[here, :], jnp.concatenate(tapers, axis=0), z3_s[e], vw_s[e])

    cell_parts = classes // chunk

    def turn(t, _):
        slot = lax.rem(t, 2)
        e = t + early

        @pl.when(t == ends[2] - early)
        def _():
            rows = collect(2)
            for k in range(ends[2] - early):
                rows = update_mine(rows, early + k, z3_s[early + k], vw_s[early + k])
            mine_s[part_rows(2), :] = rows

        @pl.when(e < batches)
        def _():
            share(e)

        @pl.when(t + 2 < batches)
        def _():
            pass_both(t + 2)

        @pl.when(t + 3 < batches)
        def _():
            shared(t + 3, recv1)

        @pl.when(t + ahead < batches)
        def _():
            send_table(t + ahead)

        @pl.when(t + 3 < batches)
        def _():
            hand_table(t + 3)

        @pl.when(t + 1 < batches)
        def _():
            near_copy(t + 1).wait_recv()
            hand_copy(t + 1).wait_recv()

        @pl.when(jnp.logical_and(t > 0, t + 1 < batches))
        def _():
            passed(t + 1)

        prior = obs_s[t].reshape(obs, LANES)
        rows = obs_s[t + 1].reshape(obs, LANES)
        coming = t + 3
        later = jnp.concatenate(
            [obs_s[coming, place].reshape(quarter, LANES) for place in (band, across)], axis=0
        )
        lat, bit = rows[:, members + 1:members + 2], rows[:, members + 4:members + 5]
        later_lat, later_bit = later[:, members + 1:members + 2], later[:, members + 4:members + 5]
        done = 0

        def some_cells(upto):
            nonlocal done
            while done < min(upto, cell_parts):
                update_cells(e - 1, done)
                done += 1

        def catch_up(later, k, z3, vw):
            return update(later, obs_taper(later_lat, later_bit, coming, e - k), z3, vw)

        lane = lane_ids(prior.shape)
        innovation = pltpu.roll(prior, LANES - 3, 1) - prior
        joined = jnp.where(lane < members, prior, jnp.where(lane == members, innovation, 0.0))
        high, low = split(joined)
        table_high = jnp.concatenate([th_s[slot, 0], th_s[slot, 1]], axis=1)
        table_low = jnp.concatenate([tl_s[slot, 0], tl_s[slot, 1]], axis=1)
        both = nn(jnp.concatenate([table_high, table_low], axis=1), tall(high, low))
        part = both[:, :LANES] + both[:, LANES:]
        lane = lane_ids((obs, LANES))
        weighted = jnp.where(lane < members, part[:obs], jnp.where(lane == members, -part[obs:], 0.0))
        vw = tall(*split(weighted * (1.0 / (members - 1.0))))
        z3 = prior_tall(prior)

        later = catch_up(later, 2, z3_s[e - 2], vw_s[e - 2])
        tapers = (obs_taper(lat, bit, t + 1, e - 1), obs_taper(later_lat, later_bit, coming, e - 1))
        both = update(jnp.concatenate([rows, later], axis=0), jnp.concatenate(tapers, axis=0), z3_s[e - 1], vw_s[e - 1])
        rows, later = both[:obs], both[obs:]
        some_cells(cell_parts)
        mine = mine_s[...]
        joint = jnp.concatenate([rows, later, mine], axis=0)
        tapers = (obs_taper(lat, bit, t + 1, e), obs_taper(later_lat, later_bit, coming, e), mine_taper(mine, e))
        joint = update(joint, jnp.concatenate(tapers, axis=0), z3, vw)
        obs_s[t + 1] = joint[:obs].reshape(obs_s.shape[1:])
        for i, place in enumerate((band, across)):
            obs_s[coming, place] = joint[obs + i * quarter:obs + (i + 1) * quarter].reshape(obs_s.shape[2:])
        mine_s[...] = joint[obs + 2 * quarter:]
        z3_s[e] = z3
        vw_s[e] = vw
        prepare(jnp.minimum(t + 1, batches - 1), 1 - slot)
        return 0

    lax.fori_loop(0, batches, turn, 0)
    for i in range(cell_parts):
        update_cells(batches - 1 + early, i)

    for p in range(3):
        for k in range(1, slabs):
            reduce_copy(k, p).wait_send()

    def sent(t, _):
        near_copy(t).wait_send()
        far_copy(t).wait_send()
        hand_copy(t).wait_send()
        return 0

    lax.fori_loop(0, batches, sent, 0)
    for s in range(ends[1]):
        pieces(s, ranks - 1, send1)

    def shared_sent(s, _):
        shared(s, send1)
        return 0

    lax.fori_loop(ends[1], batches, shared_sent, 0)


def finish_kernel(cells_ref, anom_out, mean_out):
    members, classes, levels = anom_out.shape
    for c in range(classes):
        tall = cells_ref[pl.ds(c * levels, levels), :].T
        anom_out[:, c, :] = tall[:members]
        mean_out[pl.ds(c, 1), :] = tall[members:members + 1]


def near_local(anomalies, state_mean, obs_value, obs_cell, owner, order, root_inv, gain_inv):
    members, lon_dev, lat_dev, levels = anomalies.shape
    classes = lon_dev * lat_dev
    cells = classes * levels
    batches, quarter = obs_value.shape
    obs = obs_cell.shape[1]
    half = obs // 2
    slabs, bands = lax.axis_size("gx"), lax.axis_size("gy")
    piece = quarter // slabs
    early = min(EARLY, batches)
    lat_total = float(bands * lat_dev)
    sizes = (
        members, lon_dev, lat_dev, levels, float(slabs * lon_dev), lat_total, REACH * lon_dev + 1.0, bands, slabs, early
    )
    dma = pltpu.SemaphoreType.DMA
    cells_out = pl.pallas_call(
        functools.partial(analysis_kernel, sizes),
        out_shape=jax.ShapeDtypeStruct((cells, LANES), F32),
        in_specs=[SMEM] * 3 + [VMEM] * 6,
        out_specs=VMEM,
        scratch_shapes=[
            pltpu.VMEM((batches + early, 1, obs), F32),
            pltpu.VMEM((batches + early, 1, obs), F32),
            pltpu.VMEM((quarter, LANES), F32),
            pltpu.VMEM((slabs, batches * piece, LANES), F32),
            pltpu.VMEM((slabs, batches * piece, LANES), F32),
            pltpu.VMEM((batches * piece, LANES), F32),
            pltpu.VMEM((batches, piece, LANES), F32),
            pltpu.VMEM((batches + 3, bands, slabs // 2, 2, piece, LANES), F32),
            pltpu.VMEM((batches, 2, 2, obs, half), F32),
            pltpu.VMEM((2, 2, 2 * obs, half), BF16),
            pltpu.VMEM((2, 2, 2 * obs, half), BF16),
            pltpu.VMEM((batches + early, 2 * LANES, obs), BF16),
            pltpu.VMEM((batches + early, 2 * obs, 2 * LANES), BF16),
            dma((3, slabs)), dma((3, slabs)),
            dma((batches,)), dma((batches,)),
            dma((batches, 2)), dma((batches, 2)),
            dma((3,)), dma((3,)),
            dma((batches,)), dma((batches,)),
            dma((batches,)), dma((batches,)),
            dma((batches,)), dma((batches,)),
        ],
        compiler_params=pltpu.CompilerParams(collective_id=0, has_side_effects=True),
        name="analysis",
    )(
        obs_cell, order, owner, obs_cell, obs_value,
        anomalies.reshape(members, classes, levels), state_mean.reshape(classes, levels), root_inv, gain_inv,
    )

    post, mean = pl.pallas_call(
        finish_kernel,
        out_shape=(
            jax.ShapeDtypeStruct((members, classes, levels), F32),
            jax.ShapeDtypeStruct((classes, levels), F32),
        ),
        in_specs=[VMEM],
        out_specs=(VMEM, VMEM),
        name="finish",
    )(cells_out)
    return post.reshape(members, lon_dev, lat_dev, levels), mean.reshape(lon_dev, lat_dev, levels)


def local(*arrays):
    obs_value, obs_cell = arrays[2], arrays[3]
    slabs, bands = lax.axis_size("gx"), lax.axis_size("gy")
    piece = obs_value.shape[1] // slabs
    fits = bands == 4 and piece % 8 == 0 and piece * slabs == obs_value.shape[1] and obs_cell.shape[1] == 2 * LANES
    return (near_local if fits and arrays[0].shape[1] == 2 else wide_local)(*arrays)


def solution(mesh):
    return jax.shard_map(
        local,
        mesh=mesh,
        in_specs=(
            P(None, "gx", "gy", None),
            P("gx", "gy", None),
            P(None, "gy"),
            P(),
            P(),
            P(),
            P(None, "gy", None),
            P(None, "gy", None),
        ),
        out_specs=(P(None, "gx", "gy", None), P("gx", "gy", None)),
        check_vma=False,
    )
```

```python
import functools

import jax
import jax.numpy as jnp
from jax import lax
from jax.experimental import pallas as pl
from jax.experimental.pallas import tpu as pltpu
from jax.sharding import PartitionSpec as P

REACH = 3
EARLY = 5
LANES = 128
MESH = pl.DeviceIdType.MESH
VMEM = pl.BlockSpec(memory_space=pltpu.VMEM)
SMEM = pl.BlockSpec(memory_space=pltpu.SMEM)
F32 = jnp.float32
BF16 = jnp.bfloat16


def split(value):
    high = value.astype(BF16)
    return high, (value - high.astype(F32)).astype(BF16)


def nn(left, right):
    return lax.dot_general(left, right, (((1,), (0,)), ((), ())), preferred_element_type=F32)


def nt(left, right):
    return lax.dot_general(left, right, (((1,), (1,)), ((), ())), preferred_element_type=F32)


def lane_ids(shape):
    return lax.broadcasted_iota(jnp.int32, shape, len(shape) - 1)


def pick_kernel(lon_dev, lat_dev, cells_ref, value_ref, owner_ref, order_ref, anom_ref, mean_ref, state_ref, packed_ref, rows_ref):
    column, band = lax.axis_index("gx"), lax.axis_index("gy")
    members, classes, levels = anom_ref.shape
    batches, quarter = value_ref.shape

    for c in range(classes):
        lat = (band * lat_dev + c % lat_dev).astype(F32)
        lon = (column * lon_dev + c // lat_dev).astype(F32)
        tall = jnp.concatenate(
            [
                anom_ref[:, c, :],
                mean_ref[pl.ds(c, 1), :],
                jnp.full((1, levels), lat, F32),
                jnp.full((1, levels), lon, F32),
                jnp.zeros((LANES - members - 3, levels), F32),
            ],
            axis=0,
        )
        state_ref[pl.ds(c * levels, levels), :] = tall.T

    lane = lane_ids((1, LANES))

    def batch(t, _):
        b = order_ref[t]
        mine = owner_ref[b] == column

        @pl.when(mine)
        def _():
            def group(i, _):
                for k in range(8):
                    j = i * 8 + k
                    row = state_ref[pl.ds(cells_ref[b, band * quarter + j], 1), :]
                    rows_ref[pl.ds(t * quarter + j, 1), :] = jnp.where(lane == members + 3, value_ref[b, j], row)
                return 0

            lax.fori_loop(0, quarter // 8, group, 0)

        @pl.when(jnp.logical_not(mine))
        def _():
            rows_ref[pl.ds(pl.multiple_of(t * quarter, quarter), quarter), :] = jnp.zeros((quarter, LANES), F32)

        return 0

    lax.fori_loop(0, batches, batch, 0)
    slabs, height, chunk = packed_ref.shape
    for q in range(slabs):
        packed_ref[q] = rows_ref[pl.ds(q * chunk, chunk), :].T[:height]


def spread_kernel(bands, slabs, rows_ref, out_ref, land, send1, recv1, send2, recv2, send3, recv3, send4, recv4, send5, recv5):
    x, b = lax.axis_index("gx"), lax.axis_index("gy")
    partner = b + 1 - 2 * lax.rem(b, 2)
    across = lax.rem(b + 2, bands)

    def slab(k):
        return lax.rem(x + k, slabs)

    def source(k):
        return lax.rem(x + slabs - k, slabs)

    def first(k):
        return pltpu.make_async_remote_copy(
            src_ref=rows_ref.at[slab(k)], dst_ref=land.at[k], send_sem=send1.at[k], recv_sem=recv1.at[k],
            device_id={"gx": slab(k)}, device_id_type=MESH,
        )

    def second(k):
        return pltpu.make_async_remote_copy(
            src_ref=out_ref.at[b, x], dst_ref=out_ref.at[b, x], send_sem=send2.at[k],
            recv_sem=recv2.at[k], device_id={"gx": slab(k)}, device_id_type=MESH,
        )

    def hand(k, of_band, send_sem, recv_sem, target):
        place = out_ref.at[of_band, source(k)]
        return pltpu.make_async_remote_copy(
            src_ref=place, dst_ref=place, send_sem=send_sem.at[k], recv_sem=recv_sem.at[k],
            device_id={"gy": target}, device_id_type=MESH,
        )

    def third(k):
        return hand(k, b, send3, recv3, partner)

    def fourth(k):
        return hand(k, b, send4, recv4, across)

    def fifth(k):
        return hand(k, across, send5, recv5, partner)

    def each(low, high, body):
        def step(k, _):
            body(k)
            return 0

        lax.fori_loop(low, high, step, 0)

    barrier = pltpu.get_barrier_semaphore()
    each(1, slabs, lambda k: pl.semaphore_signal(barrier, inc=1, device_id={"gx": slab(k)}, device_id_type=MESH))
    for target in (partner, across):
        pl.semaphore_signal(barrier, inc=1, device_id={"gy": target}, device_id_type=MESH)
    pl.semaphore_wait(barrier, slabs + 1)

    each(1, slabs, lambda k: first(k).start())
    out_ref[b, x] = rows_ref[x]

    def add(k):
        first(k).wait_recv()
        out_ref[b, x] += land[k]

    each(1, slabs, add)
    fourth(0).start()
    each(1, slabs, lambda k: second(k).start())
    third(0).start()

    def relay(k):
        second(k).wait_recv()
        fourth(k).start()
        third(k).start()
        fourth(k - 1).wait_recv()
        fifth(k - 1).start()

    each(1, slabs, relay)
    fourth(slabs - 1).wait_recv()
    fifth(slabs - 1).start()

    def finish(k):
        third(k).wait()
        fifth(k).wait()
        fourth(k).wait_send()

    each(0, slabs, finish)

    def sent(k):
        first(k).wait_send()
        second(k).wait_send()

    each(1, slabs, sent)


def main_kernel(
    sizes, order_ref, owner_ref, state_ref, obs_ref, cell_ref, root_ref, gain_ref,
    anom_out, mean_out,
    lat_ref, lon_ref, cells_s, obs_s, v_s, vw_s, z3_s, gh_s, gl_s, send_sem, recv_sem,
):
    members, lon_dev, lat_dev, levels, lon_total, lat_total, span, bands = sizes
    batches, obs = cell_ref.shape
    quarter = obs // bands
    column, band = lax.axis_index("gx"), lax.axis_index("gy")
    classes = lon_dev * lat_dev
    chunk = 4

    barrier = pltpu.get_barrier_semaphore()
    for k in range(1, bands):
        pl.semaphore_signal(barrier, inc=1, device_id={"gy": lax.rem(band + k, bands)}, device_id_type=MESH)
    pl.semaphore_wait(barrier, bands - 1)

    def widen(value, with_low_in_middle):
        high, low = split(value)
        high, low = high.astype(F32), low.astype(F32)
        second, third = (low, high) if with_low_in_middle else (high, low)
        lane = lane_ids(value.shape)
        room = LANES - members
        moved = pltpu.roll(second, members, 1)
        first = jnp.where(lane < members, high, moved)
        last = jnp.where(lane < members - room, moved, pltpu.roll(third, members - room, 1))
        return jnp.concatenate([first, last], axis=1), lane, room

    def state_wide(value):
        return widen(value, True)[0].astype(BF16)

    def prior_wide(value):
        wide, lane, room = widen(jnp.where(lane_ids(value.shape) < members, value, 0.0), False)
        wide_lane = lane_ids(wide.shape)
        return jnp.where(wide_lane < 3 * members, wide, 0.0).astype(BF16)

    def lon_weight(gap):
        gap = jnp.abs(gap)
        gap = jnp.minimum(gap, lon_total - gap)
        return jnp.maximum(0.0, 1.0 - gap * (1.0 / span))

    def lat_weight(gap):
        return 1.0 - jnp.abs(gap) * (1.0 / lat_total)

    def obs_taper(rows, s):
        lat, lon = rows[:, members + 1:members + 2], rows[:, members + 2:members + 3]
        return lat_weight(lat - lat_ref[s]) * lon_weight(lon - lon_ref[s])

    def apply(rows, high, low):
        both = nn(high, vw_s[...])
        return rows - (both[:, :LANES] + both[:, LANES:] + nn(low, vw_s[:, :LANES]))

    def update(rows, taper, s, slot):
        gained = nt(state_wide(rows), z3_s[slot]) * taper
        return apply(rows, *split(gained))

    def update_cells(s, slot):
        for i in range(classes // chunk):
            tapers = []
            for k in range(chunk):
                c = i * chunk + k
                lat = (band * lat_dev + c % lat_dev).astype(F32)
                lon = (column * lon_dev + c // lat_dev).astype(F32)
                weight = lat_weight(lat - lat_ref[s]) * lon_weight(lon - lon_ref[s])
                tapers.append(jnp.broadcast_to(weight, (levels, obs)))
            here = pl.ds(i * chunk * levels, chunk * levels)
            cells_s[here, :] = update(cells_s[here, :], jnp.concatenate(tapers, axis=0), s, slot)

    def at(t):
        return pl.ds(pl.multiple_of(t * obs, obs), obs)

    cells_s[...] = state_ref[...]
    _, slabs, height, width = obs_ref.shape
    part = min(width, quarter)
    for q in range(bands):
        for p in range(slabs):
            rest = jnp.zeros((LANES - height, width), F32)
            block = jnp.concatenate([obs_ref[q, p], rest], axis=0).T
            for i in range(0, width, part):
                t, j = divmod(p * width + i, quarter)
                obs_s[pl.ds(t * obs + q * quarter + j, part), :] = block[i:i + part]
    obs_s[pl.ds(batches * obs, 2 * obs), :] = jnp.zeros((2 * obs, LANES), F32)
    vw_s[...] = jnp.zeros_like(vw_s)
    z3_s[...] = jnp.zeros_like(z3_s)
    first_lat = lax.broadcasted_iota(jnp.int32, (1, obs), 1).astype(F32)
    first_lat = jnp.floor((first_lat + 0.5) * (1.0 / quarter)) * lat_dev
    for t in range(batches):
        batch_id = order_ref[t]
        level_row = jnp.floor((cell_ref[pl.ds(batch_id, 1), :].astype(F32) + 0.5) * (1.0 / levels))
        lon_row = jnp.floor((level_row + 0.5) * (1.0 / lat_dev))
        lat_ref[t] = level_row - lon_row * lat_dev + first_lat
        lon_ref[t] = lon_row + (owner_ref[batch_id] * lon_dev).astype(F32)

    def turn(t, _):
        prior = obs_s[at(t), :]
        lane = lane_ids(prior.shape)
        innovation = pltpu.roll(prior, LANES - 3, 1) - prior
        joined = jnp.where(lane < members, prior, jnp.where(lane == members, innovation, 0.0))
        high, low = split(joined)
        batch_id = order_ref[t]
        table_high, table_low = split(jnp.concatenate([root_ref[batch_id], gain_ref[batch_id]], axis=0))
        both = nn(table_high, jnp.concatenate([high, low], axis=1))
        part = both[:, :LANES] + both[:, LANES:] + nn(table_low, high)
        lane = lane_ids((quarter, LANES))
        weighted = jnp.where(lane < members, part[:quarter], jnp.where(lane == members, -part[quarter:], 0.0))
        mine = pl.ds(pl.multiple_of(band * quarter, quarter), quarter)
        v_s[t, mine, :] = weighted * (1.0 / (members - 1.0))

        def copy(k):
            return pltpu.make_async_remote_copy(
                src_ref=v_s.at[t, mine, :],
                dst_ref=v_s.at[t, mine, :],
                send_sem=send_sem.at[t, k - 1],
                recv_sem=recv_sem.at[t, k - 1],
                device_id={"gy": lax.rem(band + k, bands)},
                device_id_type=MESH,
            )

        for k in range(1, bands):
            copy(k).start()

        z3_s[lax.rem(t, 2)] = prior_wide(prior)

        before = jnp.maximum(t - 1, 0)
        past = lax.rem(t + 1, 2)
        rows = obs_s[at(t + 1), :]
        rows = update(rows, obs_taper(rows, before), before, past)
        obs_s[at(t + 1), :] = rows
        gained = nt(state_wide(rows), z3_s[lax.rem(t, 2)]) * obs_taper(rows, t)
        gh_s[...], gl_s[...] = split(gained)
        update_cells(before, past)

        def later(i, _):
            here = pl.ds(pl.multiple_of((t + 2 + 2 * i) * obs, obs), 2 * obs)
            rows = obs_s[here, :]
            obs_s[here, :] = update(rows, obs_taper(rows, before), before, past)
            return 0

        lax.fori_loop(0, (batches - 1 - t) // 2 * jnp.minimum(t, 1), later, 0)

        for k in range(1, bands):
            copy(k).wait()

        vw_s[...] = jnp.concatenate(split(v_s[t]), axis=1)

        obs_s[at(t + 1), :] = apply(obs_s[at(t + 1), :], gh_s[...], gl_s[...])
        return 0

    lax.fori_loop(0, batches, turn, 0)
    update_cells(batches - 1, (batches - 1) % 2)
    for c in range(classes):
        tall = cells_s[pl.ds(c * levels, levels), :].T
        anom_out[:, c, :] = tall[:members]
        mean_out[pl.ds(c, 1), :] = tall[members:members + 1]


def wide_local(anomalies, state_mean, obs_value, obs_cell, owner, order, root_inv, gain_inv):
    members, lon_dev, lat_dev, levels = anomalies.shape
    classes = lon_dev * lat_dev
    cells = classes * levels
    batches, quarter = obs_value.shape
    obs = obs_cell.shape[1]
    slabs, bands = lax.axis_size("gx"), lax.axis_size("gy")
    chunk = batches * quarter // slabs
    height = (members + 4 + 7) // 8 * 8
    state, rows = pl.pallas_call(
        functools.partial(pick_kernel, lon_dev, lat_dev),
        out_shape=(
            jax.ShapeDtypeStruct((cells, LANES), F32),
            jax.ShapeDtypeStruct((slabs, height, chunk), F32),
        ),
        in_specs=[SMEM] * 4 + [VMEM] * 2,
        out_specs=(VMEM, VMEM),
        scratch_shapes=[pltpu.VMEM((batches * quarter, LANES), F32)],
        name="pick",
    )(
        obs_cell, obs_value, owner, order,
        anomalies.reshape(members, classes, levels), state_mean.reshape(classes, levels),
    )

    rows = pl.pallas_call(
        functools.partial(spread_kernel, bands, slabs),
        out_shape=jax.ShapeDtypeStruct((bands, slabs, height, chunk), F32),
        in_specs=[VMEM],
        out_specs=VMEM,
        scratch_shapes=[pltpu.VMEM((slabs, height, chunk), F32)] + [pltpu.SemaphoreType.DMA((slabs,))] * 10,
        compiler_params=pltpu.CompilerParams(collective_id=1, has_side_effects=True),
        name="spread",
    )(rows)

    sizes = (
        members, lon_dev, lat_dev, levels, float(slabs * lon_dev), float(bands * lat_dev), REACH * lon_dev + 1.0, bands
    )
    post, mean = pl.pallas_call(
        functools.partial(main_kernel, sizes),
        out_shape=(
            jax.ShapeDtypeStruct((members, classes, levels), F32),
            jax.ShapeDtypeStruct((classes, levels), F32),
        ),
        in_specs=[SMEM] * 2 + [VMEM] * 5,
        out_specs=(VMEM, VMEM),
        scratch_shapes=[
            pltpu.VMEM((batches, 1, obs), F32),
            pltpu.VMEM((batches, 1, obs), F32),
            pltpu.VMEM((cells, LANES), F32),
            pltpu.VMEM(((batches + 2) * obs, LANES), F32),
            pltpu.VMEM((batches, obs, LANES), F32),
            pltpu.VMEM((obs, 2 * LANES), BF16),
            pltpu.VMEM((2, obs, 2 * LANES), BF16),
            pltpu.VMEM((obs, obs), BF16),
            pltpu.VMEM((obs, obs), BF16),
            pltpu.SemaphoreType.DMA((batches, bands - 1)),
            pltpu.SemaphoreType.DMA((batches, bands - 1)),
        ],
        compiler_params=pltpu.CompilerParams(collective_id=0, has_side_effects=True),
        name="analysis",
    )(
        order, owner, state, rows, obs_cell, root_inv, gain_inv,
    )
    return post.reshape(members, lon_dev, lat_dev, levels), mean.reshape(lon_dev, lat_dev, levels)


def analysis_kernel(
    sizes, index_ref, order_ref, owner_ref, cell_ref, value_ref, anom_ref, mean_ref, root_ref, gain_ref,
    cells_s,
    lat_ref, lon_ref, pick_s, packed_s, land, mine_s, share_s, obs_s, full_s, th_s, tl_s, z3_s, vw_s,
    rs_send, rs_recv, send1, recv1, send2, recv2, send3, recv3, near_send, near_recv, far_send, far_recv, hand_send, hand_recv,
):
    members, lon_dev, lat_dev, levels, lon_total, lat_total, span, bands, slabs, early = sizes
    batches, obs = cell_ref.shape
    quarter, half = obs // bands, obs // 2
    piece = quarter // slabs
    ahead, prompt = min(8, batches), min(6, batches)
    column, band = lax.axis_index("gx"), lax.axis_index("gy")
    partner = band + 1 - 2 * lax.rem(band, 2)
    across = lax.rem(band + bands // 2, bands)
    near = lax.div(band, bands // 2)
    far = 1 - near
    classes = lon_dev * lat_dev
    chunk = 8

    def slab(k):
        return lax.rem(column + k, slabs)

    def band_rows(b):
        return pl.ds(pl.multiple_of(b * quarter, quarter), quarter)

    def half_rows(h):
        return pl.ds(pl.multiple_of(h * half, half), half)

    def remote(src, dst, send, recv, device):
        return pltpu.make_async_remote_copy(
            src_ref=src, dst_ref=dst, send_sem=send, recv_sem=recv, device_id=device, device_id_type=MESH
        )

    ends = (0, 3, early + 2, batches)

    def part_rows(p):
        return pl.ds(ends[p] * piece, (ends[p + 1] - ends[p]) * piece)

    def reduce_copy(k, p):
        here = part_rows(p)
        return remote(
            packed_s.at[slab(k), here], land.at[k, here], rs_send.at[p, k], rs_recv.at[p, k], {"gx": slab(k)}
        )

    def my_piece(s):
        return pl.ds(pl.multiple_of(s * piece, piece), piece)

    rank, side = lax.div(column, 2), lax.rem(column, 2)
    ranks = slabs // 2

    def keep(s):
        rows = mine_s[my_piece(s), :]
        share_s[s] = rows
        obs_s[s, band, rank, side] = rows

        def start(device):
            remote(share_s.at[s], obs_s.at[s, band, rank, side], send1.at[s], recv1.at[s], device).start()

        return start

    def share_ranks(s):
        start = keep(s)
        for k in range(1, ranks):
            start({"gx": 2 * lax.rem(rank + k, ranks) + side})

    def share_sides(s):
        pieces(s, ranks - 1, recv1)
        place = obs_s.at[s, band, :, side]
        for target in ({"gx": 2 * rank + 1 - side}, {"gy": across}, {"gx": 2 * rank + 1 - side, "gy": across}):
            remote(place, place, send3.at[s], recv3.at[s], target).start()

    def share(s):
        start = keep(s)
        for k in range(slabs // 2, slabs + slabs // 2):
            start({"gx": slab(k % slabs), "gy": across})
        for k in range(1, slabs):
            start({"gx": slab((k + slabs // 2 - 1) % (slabs - 1) + 1)})

    def pieces(s, count, sem):
        window = mine_s.at[pl.ds(0, count * piece)]
        pltpu.make_async_copy(window, window, sem.at[s]).wait()

    def shared(s, sem):
        pieces(s, 2 * slabs - 1, sem)

    def pass_on(s, i):
        place = obs_s.at[s, (band, across)[i]]
        return remote(place, place, send2.at[s, i], recv2.at[s, i], {"gy": partner})

    def near_copy(t):
        return remote(
            full_s.at[t, :, :, band_rows(band)], full_s.at[t, :, :, band_rows(band)], near_send, near_recv.at[t], {"gy": partner}
        )

    def far_copy(t):
        return remote(
            full_s.at[t, :, near, band_rows(band)], full_s.at[t, :, near, band_rows(band)], far_send,
            far_recv.at[t], {"gy": across},
        )

    def hand_copy(t):
        place = full_s.at[t, :, far, band_rows(across)]
        return remote(place, place, hand_send, hand_recv.at[t], {"gy": partner})

    def send_table(t):
        far_copy(t).start()
        near_copy(t).start()

    def hand_table(t):
        far_copy(t).wait_recv()
        hand_copy(t).start()

    def prepare(t, slot):
        for k in range(2):
            aside = full_s[t, k, far, half_rows(near), :]
            blocks = (
                (near, near, full_s[t, k, near, half_rows(near), :]),
                (far, near, aside),
                (near, far, aside.T),
                (far, far, full_s[t, k, far, half_rows(far), :]),
            )
            for columns, rows, block in blocks:
                here = pl.ds(pl.multiple_of(k * obs + rows * half, half), half)
                high, low = split(block)
                th_s[slot, columns, here, :] = high
                tl_s[slot, columns, here, :] = low

    barrier = pltpu.get_barrier_semaphore()
    for k in range(1, slabs):
        pl.semaphore_signal(barrier, inc=1, device_id={"gx": slab(k)}, device_id_type=MESH)
    for k in range(slabs):
        pl.semaphore_signal(barrier, inc=1, device_id={"gx": slab(k), "gy": across}, device_id_type=MESH)
    pl.semaphore_signal(barrier, inc=1, device_id={"gy": partner}, device_id_type=MESH)

    for c in range(classes):
        lat = (band * lat_dev + c % lat_dev).astype(F32) * (1.0 / lat_total)
        lon = (column * lon_dev + c // lat_dev).astype(F32)
        tall = jnp.concatenate(
            [
                anom_ref[:, c, :],
                mean_ref[pl.ds(c, 1), :],
                jnp.full((1, levels), lat, F32),
                jnp.full((1, levels), lon, F32),
                jnp.zeros((1, levels), F32),
                jnp.full((1, levels), float(c // lat_dev), F32),
                jnp.zeros((LANES - members - 5, levels), F32),
            ],
            axis=0,
        )
        cells_s[pl.ds(c * levels, levels), :] = tall.T

    def pick(t, _):
        b = order_ref[t]
        for j in range(quarter):
            pick_s[pl.ds(j, 1), :] = cells_s[pl.ds(index_ref[b, band * quarter + j], 1), :]
        block = pick_s[...]
        values = jnp.broadcast_to(value_ref[pl.ds(b, 1), :], (LANES, quarter)).T
        block = jnp.where(lane_ids(block.shape) == members + 3, values, block)
        block = jnp.where(owner_ref[b] == column, block, 0.0)
        packed_s[:, my_piece(t), :] = block.reshape(slabs, piece, LANES)
        return 0

    def spread_part(p):
        for k in range(1, slabs):
            reduce_copy(k, p).start()

    def stage(t, _):
        b = order_ref[t]
        for h in range(2):
            full_s[t, 0, h, band_rows(band), :] = root_ref[b, :, h * half:(h + 1) * half]
            full_s[t, 1, h, band_rows(band), :] = gain_ref[b, :, h * half:(h + 1) * half]
        return 0

    lax.fori_loop(ends[0], ends[1], pick, 0)
    pl.semaphore_wait(barrier, 2 * slabs)
    spread_part(0)
    stage(0, 0)
    send_table(0)
    lax.fori_loop(ends[1], ends[2], pick, 0)
    spread_part(1)
    lax.fori_loop(1, batches, stage, 0)
    for t in range(1, prompt):
        send_table(t)
    lax.fori_loop(ends[2], ends[3], pick, 0)

    first_lat = lax.broadcasted_iota(jnp.int32, (1, obs), 1).astype(F32)
    first_lat = jnp.floor((first_lat + 0.5) * (1.0 / quarter)) * lat_dev
    for t in range(batches):
        batch_id = order_ref[t]
        level_row = jnp.floor((cell_ref[pl.ds(batch_id, 1), :].astype(F32) + 0.5) * (1.0 / levels))
        lon_row = jnp.floor((level_row + 0.5) * (1.0 / lat_dev))
        lat_ref[t + early] = (level_row - lon_row * lat_dev + first_lat) * (1.0 / lat_total)
        lon_ref[t + early] = lon_row + (owner_ref[batch_id] * lon_dev).astype(F32)
    for t in range(early):
        lat_ref[t] = jnp.zeros((1, obs), F32)
        lon_ref[t] = jnp.zeros((1, obs), F32)
        vw_s[t] = jnp.zeros(vw_s.shape[1:], BF16)
        z3_s[t] = jnp.zeros(z3_s.shape[1:], BF16)
    for s in range(batches, obs_s.shape[0]):
        obs_s[s] = jnp.zeros(obs_s.shape[1:], F32)
    mine_s[...] = jnp.zeros_like(mine_s)

    def collect(p):
        here = part_rows(p)
        total = packed_s[column, here, :]
        for k in range(1, slabs):
            reduce_copy(k, p).wait_recv()
            total = total + land[k, here, :]
        return total

    mine_s[part_rows(0), :] = collect(0)
    for s in range(ends[1]):
        share_ranks(s)
    mine_s[part_rows(1), :] = collect(1)
    for s in range(ends[1], early):
        share(s)
    spread_part(2)
    for s in range(ends[1]):
        share_sides(s)
    for t in range(prompt, ahead):
        send_table(t)
    hand_table(0)
    near_copy(0).wait_recv()
    hand_copy(0).wait_recv()
    prepare(0, 0)

    def pass_both(s):
        for i in range(2):
            pass_on(s, i).start()

    def passed(s):
        for i in range(2):
            pass_on(s, i).wait()

    for s in range(2):
        pieces(s, 3 * ranks, recv3)
        pass_both(s)
    for t in range(1, 3):
        hand_table(t)
    for s in range(2):
        passed(s)
    pieces(2, 3 * ranks, recv3)
    for s in range(ends[1]):
        pieces(s, 3 * ranks, send3)

    def state_wide(value):
        low = value - value.astype(BF16).astype(F32)
        lane = lane_ids(value.shape)
        room = LANES - members
        moved = pltpu.roll(low, members, 1)
        first = jnp.where(lane < members, value, moved)
        last = jnp.where(lane < members - room, moved, pltpu.roll(value, members - room, 1))
        return jnp.concatenate([first.astype(BF16), last.astype(BF16)], axis=1)

    def prior_tall(prior):
        high, low = split(prior.T[:members])
        return jnp.concatenate([high, high, low, jnp.zeros((2 * LANES - 3 * members, obs), BF16)], axis=0)

    def lon_weight(gap):
        gap = jnp.abs(gap)
        gap = jnp.minimum(gap, lon_total - gap)
        return jnp.maximum(0.0, 1.0 - gap * (1.0 / span))

    def lat_weight(gap):
        return 1.0 - jnp.abs(gap)

    def apply(rows, high, low, vw):
        both = nn(jnp.concatenate([high, low], axis=1), vw)
        return rows - (both[:, :LANES] + both[:, LANES:])

    def tall(high, low):
        under = jnp.concatenate([high, jnp.zeros_like(high)], axis=1)
        return jnp.concatenate([jnp.concatenate([high, low], axis=1), under], axis=0)

    def gain_of(rows, taper, z3):
        return split(nn(state_wide(rows), z3) * taper)

    def update(rows, taper, z3, vw):
        high, low = gain_of(rows, taper, z3)
        return apply(rows, high, low, vw)

    def obs_taper(lat, bit, s, e):
        lon = (owner_ref[order_ref[jnp.minimum(s, batches - 1)]] * lon_dev).astype(F32)
        west = lon_weight(lon - lon_ref[e])
        east = lon_weight(lon + 1.0 - lon_ref[e])
        return lat_weight(lat - lat_ref[e]) * (west + bit * (east - west))

    def mine_taper(rows, e):
        lat, lon = rows[:, members + 1:members + 2], rows[:, members + 2:members + 3]
        return lat_weight(lat - lat_ref[e]) * lon_weight(lon - lon_ref[e])

    def update_mine(rows, e, z3, vw):
        return update(rows, mine_taper(rows, e), z3, vw)

    def update_cells(e, part):
        tapers = []
        for k in range(chunk):
            c = part * chunk + k
            lat = (band * lat_dev + c % lat_dev).astype(F32) * (1.0 / lat_total)
            lon = (column * lon_dev + c // lat_dev).astype(F32)
            weight = lat_weight(lat - lat_ref[e]) * lon_weight(lon - lon_ref[e])
            tapers.append(jnp.broadcast_to(weight, (levels, obs)))
        here = pl.ds(part * chunk * levels, chunk * levels)
        cells_s[here, :] = update(cells_s[here, :], jnp.concatenate(tapers, axis=0), z3_s[e], vw_s[e])

    cell_parts = classes // chunk

    def turn(t, _):
        slot = lax.rem(t, 2)
        e = t + early

        @pl.when(t == ends[2] - early)
        def _():
            rows = collect(2)
            for k in range(ends[2] - early):
                rows = update_mine(rows, early + k, z3_s[early + k], vw_s[early + k])
            mine_s[part_rows(2), :] = rows

        @pl.when(e < batches)
        def _():
            share(e)

        @pl.when(t + 2 < batches)
        def _():
            pass_both(t + 2)

        @pl.when(t + 3 < batches)
        def _():
            shared(t + 3, recv1)

        @pl.when(t + ahead < batches)
        def _():
            send_table(t + ahead)

        @pl.when(t + 3 < batches)
        def _():
            hand_table(t + 3)

        @pl.when(t + 1 < batches)
        def _():
            near_copy(t + 1).wait_recv()
            hand_copy(t + 1).wait_recv()

        @pl.when(jnp.logical_and(t > 0, t + 1 < batches))
        def _():
            passed(t + 1)

        prior = obs_s[t].reshape(obs, LANES)
        rows = obs_s[t + 1].reshape(obs, LANES)
        coming = t + 3
        later = jnp.concatenate(
            [obs_s[coming, place].reshape(quarter, LANES) for place in (band, across)], axis=0
        )
        lat, bit = rows[:, members + 1:members + 2], rows[:, members + 4:members + 5]
        later_lat, later_bit = later[:, members + 1:members + 2], later[:, members + 4:members + 5]
        done = 0

        def some_cells(upto):
            nonlocal done
            while done < min(upto, cell_parts):
                update_cells(e - 1, done)
                done += 1

        def catch_up(later, k, z3, vw):
            return update(later, obs_taper(later_lat, later_bit, coming, e - k), z3, vw)

        lane = lane_ids(prior.shape)
        innovation = pltpu.roll(prior, LANES - 3, 1) - prior
        joined = jnp.where(lane < members, prior, jnp.where(lane == members, innovation, 0.0))
        high, low = split(joined)
        table_high = jnp.concatenate([th_s[slot, 0], th_s[slot, 1]], axis=1)
        table_low = jnp.concatenate([tl_s[slot, 0], tl_s[slot, 1]], axis=1)
        both = nn(jnp.concatenate([table_high, table_low], axis=1), tall(high, low))
        part = both[:, :LANES] + both[:, LANES:]
        lane = lane_ids((obs, LANES))
        weighted = jnp.where(lane < members, part[:obs], jnp.where(lane == members, -part[obs:], 0.0))
        vw = tall(*split(weighted * (1.0 / (members - 1.0))))
        z3 = prior_tall(prior)

        later = catch_up(later, 2, z3_s[e - 2], vw_s[e - 2])
        tapers = (obs_taper(lat, bit, t + 1, e - 1), obs_taper(later_lat, later_bit, coming, e - 1))
        both = update(jnp.concatenate([rows, later], axis=0), jnp.concatenate(tapers, axis=0), z3_s[e - 1], vw_s[e - 1])
        rows, later = both[:obs], both[obs:]
        some_cells(cell_parts)
        mine = mine_s[...]
        joint = jnp.concatenate([rows, later, mine], axis=0)
        tapers = (obs_taper(lat, bit, t + 1, e), obs_taper(later_lat, later_bit, coming, e), mine_taper(mine, e))
        joint = update(joint, jnp.concatenate(tapers, axis=0), z3, vw)
        obs_s[t + 1] = joint[:obs].reshape(obs_s.shape[1:])
        for i, place in enumerate((band, across)):
            obs_s[coming, place] = joint[obs + i * quarter:obs + (i + 1) * quarter].reshape(obs_s.shape[2:])
        mine_s[...] = joint[obs + 2 * quarter:]
        z3_s[e] = z3
        vw_s[e] = vw
        prepare(jnp.minimum(t + 1, batches - 1), 1 - slot)
        return 0

    lax.fori_loop(0, batches, turn, 0)
    for i in range(cell_parts):
        update_cells(batches - 1 + early, i)

    for p in range(3):
        for k in range(1, slabs):
            reduce_copy(k, p).wait_send()

    for window, sem in (
        (full_s.at[:, :, :, band_rows(band)], near_send),
        (full_s.at[:, :, near, band_rows(band)], far_send),
        (full_s.at[:, :, far, band_rows(across)], hand_send),
    ):
        pltpu.make_async_copy(window, window, sem).wait()
    for s in range(ends[1]):
        pieces(s, ranks - 1, send1)

    def shared_sent(s, _):
        shared(s, send1)
        return 0

    lax.fori_loop(ends[1], batches, shared_sent, 0)


def finish_kernel(cells_ref, anom_out, mean_out):
    members, classes, levels = anom_out.shape
    for c in range(classes):
        tall = cells_ref[pl.ds(c * levels, levels), :].T
        anom_out[:, c, :] = tall[:members]
        mean_out[pl.ds(c, 1), :] = tall[members:members + 1]


def near_local(anomalies, state_mean, obs_value, obs_cell, owner, order, root_inv, gain_inv):
    members, lon_dev, lat_dev, levels = anomalies.shape
    classes = lon_dev * lat_dev
    cells = classes * levels
    batches, quarter = obs_value.shape
    obs = obs_cell.shape[1]
    half = obs // 2
    slabs, bands = lax.axis_size("gx"), lax.axis_size("gy")
    piece = quarter // slabs
    early = min(EARLY, batches)
    lat_total = float(bands * lat_dev)
    sizes = (
        members, lon_dev, lat_dev, levels, float(slabs * lon_dev), lat_total, REACH * lon_dev + 1.0, bands, slabs, early
    )
    dma = pltpu.SemaphoreType.DMA
    cells_out = pl.pallas_call(
        functools.partial(analysis_kernel, sizes),
        out_shape=jax.ShapeDtypeStruct((cells, LANES), F32),
        in_specs=[SMEM] * 3 + [VMEM] * 6,
        out_specs=VMEM,
        scratch_shapes=[
            pltpu.VMEM((batches + early, 1, obs), F32),
            pltpu.VMEM((batches + early, 1, obs), F32),
            pltpu.VMEM((quarter, LANES), F32),
            pltpu.VMEM((slabs, batches * piece, LANES), F32),
            pltpu.VMEM((slabs, batches * piece, LANES), F32),
            pltpu.VMEM((batches * piece, LANES), F32),
            pltpu.VMEM((batches, piece, LANES), F32),
            pltpu.VMEM((batches + 3, bands, slabs // 2, 2, piece, LANES), F32),
            pltpu.VMEM((batches, 2, 2, obs, half), F32),
            pltpu.VMEM((2, 2, 2 * obs, half), BF16),
            pltpu.VMEM((2, 2, 2 * obs, half), BF16),
            pltpu.VMEM((batches + early, 2 * LANES, obs), BF16),
            pltpu.VMEM((batches + early, 2 * obs, 2 * LANES), BF16),
            dma((3, slabs)), dma((3, slabs)),
            dma((batches,)), dma((batches,)),
            dma((batches, 2)), dma((batches, 2)),
            dma((3,)), dma((3,)),
            dma, dma((batches,)),
            dma, dma((batches,)),
            dma, dma((batches,)),
        ],
        compiler_params=pltpu.CompilerParams(collective_id=0, has_side_effects=True),
        name="analysis",
    )(
        obs_cell, order, owner, obs_cell, obs_value,
        anomalies.reshape(members, classes, levels), state_mean.reshape(classes, levels), root_inv, gain_inv,
    )

    post, mean = pl.pallas_call(
        finish_kernel,
        out_shape=(
            jax.ShapeDtypeStruct((members, classes, levels), F32),
            jax.ShapeDtypeStruct((classes, levels), F32),
        ),
        in_specs=[VMEM],
        out_specs=(VMEM, VMEM),
        name="finish",
    )(cells_out)
    return post.reshape(members, lon_dev, lat_dev, levels), mean.reshape(lon_dev, lat_dev, levels)


def local(*arrays):
    obs_value, obs_cell = arrays[2], arrays[3]
    slabs, bands = lax.axis_size("gx"), lax.axis_size("gy")
    piece = obs_value.shape[1] // slabs
    fits = bands == 4 and piece % 8 == 0 and piece * slabs == obs_value.shape[1] and obs_cell.shape[1] == 2 * LANES
    return (near_local if fits and arrays[0].shape[1] == 2 else wide_local)(*arrays)


def solution(mesh):
    return jax.shard_map(
        local,
        mesh=mesh,
        in_specs=(
            P(None, "gx", "gy", None),
            P("gx", "gy", None),
            P(None, "gy"),
            P(),
            P(),
            P(),
            P(None, "gy", None),
            P(None, "gy", None),
        ),
        out_specs=(P(None, "gx", "gy", None), P("gx", "gy", None)),
        check_vma=False,
    )
```
